128 devices in a mesh: row: 8 (over x, core), col: 16 (over y, z).
Axes of the slice: x: 4, y: 4, z: 4, core: 2. Of those that a mesh axis runs over, the one named last changes fastest.
Arguments:
- tiles: bfloat16 [8, 16, 128, 128, 128], P('row', 'col')
- tile_row: int32 [8, 16, 128], P('row', 'col'), may hold values from 0 to 15, as said below
- tile_col: int32 [8, 16, 128], P('row', 'col'), may hold values from 0 to 15
- tile_count: int32 [8, 16], P('row', 'col'), may hold values from 1 to 128, as said below
- sinogram: float32 [8, 2048, 128], P('row', 'col')
Outputs:
- volume: float32 [16, 2048, 128], P('col', 'row')
- residual: float32 [8, 2048, 128], P('row', 'col')
The draws below stay inside these ranges and needn't reach their ends.
Inputs may be any that keep to these rules, and one draw needn't show every extreme that they name: Within one block the pairs (tile_row, tile_col) of all 128 slots are distinct. Slots 0 to tile_count - 1 of a block are live, the rest are ignored; some block has all 128 slots live in every draw.
All inputs are finite; a program needn't handle non-finite values.
Results may differ from the reference program's by a relative error of at most 0.015.
Values may be sent and summed in bfloat16 or wider, within the bound.
No kernel may reach another device: no remote copies, remote signals or barrier semaphores. Data moves between devices by JAX's collectives and lax.ppermute only.
A program may use at most 64 MiB of HBM per device.

```python
import jax
import jax.numpy as jnp
from jax import lax

TILE = 128
RT = 16
VT = 16
TMAX = 128
FRAMES = 128
ITERS = 4
RAYS = 2048
VOX = 2048
N_ROW = 8
N_COL = 16


def tile_pairs(key):
    keys = jax.random.split(jax.random.fold_in(key, 7), N_ROW * N_COL)

    def shuffled(single):
        return jax.random.permutation(single, jnp.arange(RT * VT, dtype=jnp.int32))
    order = jax.vmap(shuffled)(keys)[:, :TMAX]
    rows = (order // VT).reshape(N_ROW, N_COL, TMAX).astype(jnp.int32)
    cols = (order % VT).reshape(N_ROW, N_COL, TMAX).astype(jnp.int32)
    return (rows, cols)


def draw_tile_row(key, part):
    return tile_pairs(key)[0]


def draw_tile_col(key, part):
    return tile_pairs(key)[1]


def draw_tile_count(key, part):
    base = TMAX // 8 + jax.random.randint(jax.random.fold_in(key, 3), (N_ROW * N_COL,), 0, TMAX // 2 + 1)
    base = jnp.maximum(base, 1)
    fullest = jax.random.randint(jax.random.fold_in(key, 5), (), 0, N_ROW * N_COL)
    base = jnp.where(jnp.arange(N_ROW * N_COL, dtype=jnp.int32) == fullest, TMAX, base)
    return base.reshape(N_ROW, N_COL).astype(jnp.int32)


def draw_tiles(key, part):
    shape = (N_ROW, N_COL, TMAX, TILE, TILE)
    place = lax_index(shape)
    rising = 3.0 ** (place / max(N_ROW * N_COL - 1, 1))
    fan = (TILE * N_COL * TMAX // (2 * RT)) ** (-0.5)
    values = jax.random.normal(jax.random.fold_in(key, 11), shape, jnp.float32)
    return (values * rising * fan).astype(jnp.bfloat16)


def lax_index(shape):
    first = jax.lax.broadcasted_iota(jnp.float32, shape, 0)
    second = jax.lax.broadcasted_iota(jnp.float32, shape, 1)
    return first * N_COL + second


def draw_sinogram(key, part):
    shape = (N_ROW, RAYS, FRAMES)
    ray = jax.lax.broadcasted_iota(jnp.float32, shape, 0) * RAYS + jax.lax.broadcasted_iota(jnp.float32, shape, 1)
    rising = 3.0 ** (ray / (N_ROW * RAYS - 1))
    values = jnp.clip(jax.random.normal(jax.random.fold_in(key, 17), shape, jnp.float32), -6.0, 6.0)
    return values * rising * 0.25


def setup_inputs(seed: int = 0) -> dict:
    key_of = jax.random.split(jax.random.key(seed), 6)
    return {
        "tiles": draw_tiles(jax.random.fold_in(key_of[5], 71), 0),
        "tile_row": draw_tile_row(jax.random.fold_in(key_of[5], 71), 0),
        "tile_col": draw_tile_col(jax.random.fold_in(key_of[5], 71), 0),
        "tile_count": draw_tile_count(jax.random.fold_in(key_of[5], 71), 0),
        "sinogram": draw_sinogram(jax.random.fold_in(key_of[5], 71), 0),
    }


def tile_pick(table, index):
    return lax.optimization_barrier(jnp.take(table, index, axis=0))


def forward_block(blocks, rows_index, cols_index, count, voxel_tiles):
    picked = tile_pick(voxel_tiles, cols_index)
    products = jnp.einsum("tij,tjk->tik", blocks.astype(jnp.float32), picked.astype(jnp.float32))
    live = jnp.arange(TMAX, dtype=jnp.int32) < count
    select = ((rows_index[None, :] == jnp.arange(RT, dtype=jnp.int32)[:, None]) & live[None, :]).astype(jnp.float32)
    return jnp.einsum("ut,tik->uik", select, products, precision=lax.Precision.HIGHEST)


def backward_block(blocks, rows_index, cols_index, count, ray_tiles):
    picked = tile_pick(ray_tiles, rows_index)
    products = jnp.einsum("tji,tjk->tik", blocks.astype(jnp.float32), picked.astype(jnp.float32))
    live = jnp.arange(TMAX, dtype=jnp.int32) < count
    select = ((cols_index[None, :] == jnp.arange(VT, dtype=jnp.int32)[:, None]) & live[None, :]).astype(jnp.float32)
    return jnp.einsum("ut,tik->uik", select, products, precision=lax.Precision.HIGHEST)


def reference(tiles, tile_row, tile_col, tile_count, sinogram):
    blocks_all = tiles.reshape(N_ROW * N_COL, TMAX, TILE, TILE)
    rows_all = tile_row.reshape(N_ROW * N_COL, TMAX)
    cols_all = tile_col.reshape(N_ROW * N_COL, TMAX)
    counts_all = tile_count.reshape(N_ROW * N_COL)
    devices = jnp.arange(N_ROW * N_COL, dtype=jnp.int32)

    def apply_forward(direction):
        voxel_tiles = direction.astype(jnp.bfloat16).reshape(N_COL, VT, TILE, FRAMES)

        def single(device):
            return forward_block(blocks_all[device], rows_all[device], cols_all[device],
                                 counts_all[device], voxel_tiles[device % N_COL])

        parts = lax.map(single, devices)
        return parts.reshape(N_ROW, N_COL, RAYS, FRAMES).sum(axis=1)

    def apply_backward(field):
        ray_tiles = field.astype(jnp.bfloat16).reshape(N_ROW, RT, TILE, FRAMES)

        def single(device):
            return backward_block(blocks_all[device], rows_all[device], cols_all[device],
                                  counts_all[device], ray_tiles[device // N_COL])

        parts = lax.map(single, devices)
        return parts.reshape(N_ROW, N_COL, VOX, FRAMES).sum(axis=0)

    volume = jnp.zeros((N_COL, VOX, FRAMES), jnp.float32)
    residual = sinogram
    search = apply_backward(residual)
    gamma = jnp.sum(search * search, axis=(0, 1))
    direction = search
    for step in range(ITERS):
        image = apply_forward(direction)
        alpha = gamma / jnp.sum(image * image, axis=(0, 1))
        volume = volume + alpha * direction
        residual = residual - alpha * image
        if step + 1 < ITERS:
            search = apply_backward(residual)
            fresh = jnp.sum(search * search, axis=(0, 1))
            direction = search + (fresh / gamma) * direction
            gamma = fresh
    return volume, residual
```

```python
import jax
import jax.numpy as jnp
from jax import lax
from jax.experimental import pallas as pl
from jax.experimental.pallas import tpu as pltpu
from jax.sharding import Mesh
from jax.sharding import PartitionSpec as P

ROW = ("x", "k")
COL = ("y", "z")
NX, NK, NC = 4, 2, 16
TILE = 128
RAYS = 2048
VOX = 2048
FRAMES = 128
ITERS = 4
RS = RAYS // NC
VS = VOX // (NX * NK)
PAD = 16
BF = jnp.bfloat16
F32 = jnp.float32


def vmem():
    return pl.BlockSpec(memory_space=pltpu.VMEM)


def smem():
    return pl.BlockSpec(memory_space=pltpu.SMEM)


def shape(dims, dtype):
    return jax.ShapeDtypeStruct(dims, dtype)


def kernel(body, name, outs, ins, scratch=(), limit=8):
    return pl.pallas_call(
        body,
        name=name,
        out_shape=outs,
        in_specs=[smem() if a.dtype == jnp.int32 else vmem() for a in ins],
        out_specs=jax.tree.map(lambda _: vmem(), outs),
        scratch_shapes=list(scratch),
        compiler_params=pltpu.CompilerParams(vmem_limit_bytes=limit << 20),
    )(*ins)


def as_rows(row):
    high = row.astype(BF).astype(F32)
    rest = row - high
    mid = rest.astype(BF).astype(F32)
    low = rest - mid
    i = lax.broadcasted_iota(jnp.int32, (PAD, FRAMES), 0)
    zero = jnp.zeros((PAD, FRAMES), F32)
    return jnp.where(i == 0, high, jnp.where(i == 1, mid, jnp.where(i == 2, low, zero))).astype(BF)


def row_of(rows):
    return jnp.sum(rows.astype(F32), axis=0, keepdims=True)


def wide(row):
    return jnp.broadcast_to(row, (8, FRAMES))


def squares(values):
    return jnp.sum(values * values, axis=0, keepdims=True)


def build_body(rows, cols, count, tiles, dense, sem):
    dense[...] = jnp.zeros_like(dense)
    live = count[0]

    def copy(t):
        r = pl.multiple_of(rows[t] * TILE, TILE)
        c = pl.multiple_of(cols[t] * TILE, TILE)
        return pltpu.make_async_copy(tiles.at[t], dense.at[pl.ds(r, TILE), pl.ds(c, TILE)], sem)

    def start(t, carry):
        copy(t).start()
        return carry

    def wait(t, carry):
        copy(t).wait()
        return carry

    lax.fori_loop(0, live, start, 0)
    lax.fori_loop(0, live, wait, 0)


def build(rows, cols, count, tiles):
    return pl.pallas_call(
        build_body,
        name="build",
        out_shape=pltpu.VMEM((RAYS, VOX), BF),
        in_specs=[smem(), smem(), smem(), pl.BlockSpec(memory_space=pltpu.HBM)],
        out_specs=vmem(),
        scratch_shapes=[pltpu.SemaphoreType.DMA(())],
        compiler_params=pltpu.CompilerParams(vmem_limit_bytes=24 << 20),
    )(rows, cols, count, tiles)


def send_all(message, values, norm):
    piece = jnp.concatenate([values.astype(BF), as_rows(norm)], axis=0)
    for c in range(NC):
        message[c] = piece


def start_body(sino, message):
    values = sino[...]
    send_all(message, values, squares(values))


def backward_body(k, arrived, dense, send, keep, norm, field, total):
    for c in range(NC):
        field[c * RS : (c + 1) * RS] = arrived[c, :RS]
    seen = arrived[0, RS:].astype(F32)
    for c in range(1, NC):
        seen += arrived[c, RS:].astype(F32)
    row = jnp.sum(seen, axis=0, keepdims=True)
    norm[...] = wide(row)
    total[...] = lax.dot_general(
        dense[...], field[...], (((0,), (0,)), ((), ())), preferred_element_type=F32
    )
    mine = k[0]
    for x in range(NX):
        here = pl.multiple_of((NK * x + mine) * VS, VS)
        there = pl.multiple_of((NK * x + 1 - mine) * VS, VS)
        keep[x] = total[pl.ds(here, VS)]
        send[x * VS : (x + 1) * VS] = total[pl.ds(there, VS)].astype(BF)
    send[NX * VS :] = as_rows(row)


def pair_body(x, keep, other, norm, own, both, *pieces):
    row = norm[0:1] + row_of(other[NX * VS :])
    both[...] = wide(row)
    rows = as_rows(row)
    for j in range(NX):
        at = (x[0] + j) % NX
        start = pl.multiple_of(at * VS, VS)
        value = keep[at] + other[pl.ds(start, VS)].astype(F32)
        if j == 0:
            own[...] = value
        else:
            pieces[j - 1][:VS] = value.astype(BF)
            pieces[j - 1][VS:] = rows


def arrived_sum(own, both, pieces):
    value = own[...]
    row = both[0:1]
    for p in pieces:
        value = value + p[:VS].astype(F32)
        row = row + row_of(p[VS:])
    return value, row


def put_search(message, search):
    message[:VS] = search.astype(BF)
    message[VS:] = as_rows(squares(search))


def first_body(own, both, p1, p2, p3, search, message, norm):
    value, row = arrived_sum(own, both, (p1, p2, p3))
    search[...] = value
    put_search(message, value)
    norm[...] = wide(row)


def next_body(
    own, both, p1, p2, p3, old, way, vol, res, image, gamma, beta, guess,
    search, direction, volume, residual, message, step,
):
    value, row = arrived_sum(own, both, (p1, p2, p3))
    alpha = gamma[0:1] / row
    ratio = alpha / guess[0:1]
    fresh = (1.0 - ratio) * old[...] + ratio * value
    search[...] = fresh
    put_search(message, fresh)
    along = old[...] + beta[0:1] * way[...]
    direction[...] = along
    volume[...] = vol[...] + alpha * along
    residual[...] = res[...] - alpha * image[...]
    step[...] = wide(alpha)


def forward_body(x, k, *refs):
    direct, swapped = refs[:NX], refs[NX : 2 * NX]
    dense, out, field, total = refs[2 * NX :]
    row = jnp.zeros((1, FRAMES), F32)
    for parts, core in ((direct, k[0]), (swapped, 1 - k[0])):
        for j in range(NX):
            at = (x[0] + NX - j) % NX
            start = pl.multiple_of((NK * at + core) * VS, VS)
            field[pl.ds(start, VS)] = parts[j][:VS]
            row = row + row_of(parts[j][VS:])
    total[...] = lax.dot_general(
        dense[...], field[...], (((1,), (0,)), ((), ())), preferred_element_type=F32
    )
    rows = as_rows(row)
    for c in range(NC):
        out[c, :RS] = total[c * RS : (c + 1) * RS].astype(BF)
        out[c, RS:] = rows


def gathered(arrived):
    value = arrived[0].astype(F32)
    for c in range(1, NC):
        value = value + arrived[c].astype(F32)
    return value[:RS], jnp.sum(value[RS:], axis=0, keepdims=True)


def image_first_body(arrived, res, last, image, gamma, guess, message):
    value, row = gathered(arrived)
    image[...] = value
    gamma[...] = wide(row)
    about = last[0:1] / row
    about = jnp.where((about > 0.0) & (about < jnp.inf), about, 1.0)
    guess[...] = wide(about)
    send_all(message, res[...] - about * value, squares(value))


def image_next_body(arrived, res, about, previous, last, image, gamma, beta, message):
    value, row = gathered(arrived)
    ratio = row / last[0:1]
    value = value + ratio * previous[...]
    image[...] = value
    gamma[...] = wide(row)
    beta[...] = wide(ratio)
    send_all(message, res[...] - about[0:1] * value, squares(value))


def image_last_body(arrived, previous, last, image, gamma, beta, norm):
    value, row = gathered(arrived)
    ratio = row / last[0:1]
    value = value + ratio * previous[...]
    image[...] = value
    gamma[...] = wide(row)
    beta[...] = wide(ratio)
    norm[...] = wide(squares(value))


def final_body(norms, gamma, search, beta, way, vol, res, image, volume, residual):
    total = norms[0, 0:1]
    for r in range(1, NX * NK):
        total = total + norms[r, 0:1]
    alpha = gamma[0:1] / total
    volume[...] = vol[...] + alpha * (search[...] + beta[0:1] * way[...])
    residual[...] = res[...] - alpha * image[...]


def shifted(value, axis, by):
    n = lax.axis_size(axis)
    return lax.ppermute(value, axis, [(i, (i + by) % n) for i in range(n)])


def exchanged(parts, axis):
    return lax.all_to_all(parts, axis, split_axis=0, concat_axis=0, tiled=True)


def to_all(part, axis):
    return exchanged(jnp.broadcast_to(part, (lax.axis_size(axis), *part.shape)), axis)


LINE = (8, FRAMES)
COLUMN = (NC, RS + PAD, FRAMES)
SHARD = (VS + PAD, FRAMES)


def local(tiles, tile_row, tile_col, tile_count, sinogram):
    x = lax.axis_index("x").astype(jnp.int32).reshape(1)
    k = lax.axis_index("k").astype(jnp.int32).reshape(1)
    dense = build(tile_row[0, 0], tile_col[0, 0], tile_count[0], tiles[0, 0])
    line = shape(LINE, F32)
    rays = shape((RS, FRAMES), F32)
    voxels = shape((VS, FRAMES), F32)
    column = shape(COLUMN, BF)
    shard = shape(SHARD, BF)

    def backward(message):
        arrived = exchanged(message, COL)
        send, keep, norm = kernel(
            backward_body,
            "backward",
            (shape((NX * VS + PAD, FRAMES), BF), shape((NX, VS, FRAMES), F32), line),
            (k, arrived, dense),
            (pltpu.VMEM((RAYS, FRAMES), BF), pltpu.VMEM((VOX, FRAMES), F32)),
            24,
        )
        other = shifted(send, "k", 1)
        own, both, *pieces = kernel(
            pair_body, "pair", (voxels, line, shard, shard, shard), (x, keep, other, norm)
        )
        far = shifted(pieces[1], "x", 2)
        near = shifted(pieces[0], "x", 1)
        back = shifted(pieces[2], "x", 3)
        return own, both, near, far, back

    def forward(message):
        far = shifted(message, "x", 2)
        near = shifted(message, "x", 1)
        back = shifted(message, "x", 3)
        direct = (message, near, far, back)
        swapped = tuple(shifted(p, "k", 1) for p in direct)
        out = kernel(
            forward_body,
            "forward",
            column,
            (x, k, *direct, *swapped, dense),
            (pltpu.VMEM((VOX, FRAMES), BF), pltpu.VMEM((RAYS, FRAMES), F32)),
            24,
        )
        return exchanged(out, COL)

    residual = sinogram[0]
    message = kernel(start_body, "start", column, (residual,))
    search, shard_out, last = kernel(
        first_body, "first", (voxels, shard, line), backward(message)
    )
    direction = jnp.zeros((VS, FRAMES), F32)
    volume = direction
    image, gamma, guess, message = kernel(
        image_first_body,
        "image_first",
        (rays, line, line, column),
        (forward(shard_out), residual, last),
    )
    beta = jnp.zeros(LINE, F32)
    for step in range(1, ITERS):
        search, direction, volume, residual, shard_out, guess = kernel(
            next_body,
            "next",
            (voxels, voxels, voxels, rays, shard, line),
            (
                *backward(message),
                search, direction, volume, residual, image, gamma, beta, guess,
            ),
        )
        arrived = forward(shard_out)
        if step + 1 < ITERS:
            image, gamma, beta, message = kernel(
                image_next_body,
                "image_next",
                (rays, line, line, column),
                (arrived, residual, guess, image, gamma),
            )
    image, gamma, beta, norm = kernel(
        image_last_body, "image_last", (rays, line, line, line), (arrived, image, gamma)
    )
    norms = to_all(to_all(norm, COL).sum(axis=0), ROW)
    volume, residual = kernel(
        final_body,
        "final",
        (voxels, rays),
        (norms, gamma, search, beta, direction, volume, residual, image),
    )
    return volume[None], residual[None]


def solution(mesh):
    finer = Mesh(mesh.devices.reshape(4, 2, 4, 4), ("x", "k", "y", "z"))
    placed = (
        P(ROW, COL, None, None, None),
        P(ROW, COL, None),
        P(ROW, COL, None),
        P(ROW, COL),
        P(ROW, COL, None),
    )
    return jax.shard_map(
        local,
        mesh=finer,
        in_specs=placed,
        out_specs=(P(COL, ROW, None), P(ROW, COL, None)),
        check_vma=False,
    )
```

```python
import jax
import jax.numpy as jnp
from jax import lax
from jax.experimental import pallas as pl
from jax.experimental.pallas import tpu as pltpu
from jax.sharding import Mesh
from jax.sharding import PartitionSpec as P

ROW = ("x", "k")
COL = ("y", "z")
NX, NK, NC = 4, 2, 16
TILE = 128
RAYS = 2048
VOX = 2048
FRAMES = 128
ITERS = 4
FH = FRAMES // NK
RS = RAYS // NC
RO = NK * RS
VS = VOX // NX
VH = VS // NK
PAD = 8
LANES = 128
BF = jnp.bfloat16
F32 = jnp.float32


def vmem():
    return pl.BlockSpec(memory_space=pltpu.VMEM)


def smem():
    return pl.BlockSpec(memory_space=pltpu.SMEM)


def hbm():
    return pl.BlockSpec(memory_space=pltpu.HBM)


def shape(dims, dtype):
    return jax.ShapeDtypeStruct(dims, dtype)


def kernel(body, name, outs, ins, scratch=(), limit=4):
    return pl.pallas_call(
        body,
        name=name,
        out_shape=outs,
        in_specs=[smem() if a.dtype == jnp.int32 else vmem() for a in ins],
        out_specs=jax.tree.map(lambda _: vmem(), outs),
        scratch_shapes=list(scratch),
        compiler_params=pltpu.CompilerParams(vmem_limit_bytes=limit << 20),
    )(*ins)


def squares(values):
    total = values[:, :LANES] * values[:, :LANES]
    for i in range(LANES, values.shape[1], LANES):
        total += values[:, i : i + LANES] * values[:, i : i + LANES]
    square = jnp.concatenate([total, jnp.zeros((LANES - FH, LANES), F32)], axis=0)
    return jnp.sum(square.T, axis=0, keepdims=True)


def per_frame(row, width):
    column = jnp.broadcast_to(row, (LANES, LANES)).T[:FH]
    return jnp.concatenate([column] * (width // LANES), axis=1)


def as_rows(row, width):
    high = row.astype(BF).astype(F32)
    rest = row - high
    mid = rest.astype(BF).astype(F32)
    low = rest - mid
    i = lax.broadcasted_iota(jnp.int32, (PAD, LANES), 0)
    zero = jnp.zeros((PAD, LANES), F32)
    rows = jnp.where(i == 0, high, jnp.where(i == 1, mid, jnp.where(i == 2, low, zero)))
    return jnp.concatenate([rows, jnp.zeros((PAD, width - LANES), F32)], axis=1).astype(BF)


def row_of(rows):
    return jnp.sum(rows[:, :LANES].astype(F32), axis=0, keepdims=True)


def wide(row):
    return jnp.broadcast_to(row, (8, LANES))


def put(message, values, row):
    message[:FH] = values.astype(BF)
    message[FH:] = as_rows(row, message.shape[1])


def put_all(message, values, row):
    part = values.astype(BF)
    rows = as_rows(row, RO)
    for c in range(NC):
        message[c, :FH] = part
        message[c, FH:] = rows


def turn_body(k, sino, mine, other, turned):
    turned[...] = sino[...].T
    mine[...] = turned[pl.ds(pl.multiple_of(k[0] * FH, FH), FH)]
    other[...] = turned[pl.ds(pl.multiple_of((1 - k[0]) * FH, FH), FH)]


def start_body(mine, other, residual, message):
    values = jnp.concatenate([mine[...], other[...]], axis=1)
    residual[...] = values
    put_all(message, values, squares(values))


def build_body(x, table, table2, tiles, tiles2, after, dense, sem):
    dense[...] = jnp.zeros_like(dense)
    shift = x[0] * (NC // NX)

    def copy(half, t):
        index, stored = ((table, tiles), (table2, tiles2))[half]
        r = pl.multiple_of(index[0, t] * TILE + half * RAYS, TILE)
        c = pl.multiple_of((index[1, t] + NC - shift) % NC * TILE, TILE)
        return pltpu.make_async_copy(stored.at[t], dense.at[pl.ds(r, TILE), pl.ds(c, TILE)], sem)

    def start(half):
        def step(t, carry):
            copy(half, t).start()
            return carry

        return step

    def wait(half):
        def step(t, carry):
            copy(half, t).wait()
            return carry

        return step

    lax.fori_loop(0, table[2, 0], start(0), 0)
    lax.fori_loop(0, table2[2, 0], start(1), 0)
    lax.fori_loop(0, table[2, 0], wait(0), 0)
    lax.fori_loop(0, table2[2, 0], wait(1), 0)


def build(x, table, table2, tiles, tiles2, after):
    return pl.pallas_call(
        build_body,
        name="build",
        out_shape=pltpu.VMEM((NK * RAYS, VOX), BF),
        in_specs=[smem(), smem(), smem(), hbm(), hbm(), vmem()],
        out_specs=vmem(),
        scratch_shapes=[pltpu.SemaphoreType.DMA(())],
        compiler_params=pltpu.CompilerParams(vmem_limit_bytes=24 << 20),
    )(x, table, table2, tiles, tiles2, after)


def backward_body(arrived, dense, own, norm, p1, p2, p3, field):
    seen = arrived[0, FH:].astype(F32)
    for c in range(NC):
        part = arrived[c, :FH]
        for h in range(NK):
            field[:, h * RAYS + c * RS : h * RAYS + (c + 1) * RS] = part[:, h * RS : (h + 1) * RS]
        if c:
            seen += arrived[c, FH:].astype(F32)
    row = row_of(seen)
    norm[...] = wide(row)
    for j, out in enumerate((own, p1, p2, p3)):
        part = jnp.dot(
            field[...], dense[:, j * VS : (j + 1) * VS], preferred_element_type=F32
        )
        if j == 0:
            out[...] = part
        else:
            put(out, part, row)


def arrived_sum(own, norm, pieces):
    value = own[...]
    row = norm[0:1]
    for p in pieces:
        value = value + p[:FH].astype(F32)
        row = row + row_of(p[FH:])
    return value, row


def first_body(own, norm, p1, p2, p3, search, message, total):
    value, row = arrived_sum(own, norm, (p1, p2, p3))
    search[...] = value
    put(message, value, squares(value))
    total[...] = wide(row)


def next_body(first, own, norm, p1, p2, p3, *refs):
    if first:
        old, res, image, gamma, guess = refs[:5]
        outs = refs[5:]
    else:
        old, res, image, gamma, guess, beta, way, vol = refs[:8]
        outs = refs[8:]
    search, direction, volume, residual, message, step = outs
    value, row = arrived_sum(own, norm, (p1, p2, p3))
    alpha = gamma[0:1] / row
    ratio = per_frame(alpha / guess[0:1], VS)
    fresh = (1.0 - ratio) * old[...] + ratio * value
    search[...] = fresh
    put(message, fresh, squares(fresh))
    scale = per_frame(alpha, VS)
    if first:
        along = old[...]
        volume[...] = scale * along
    else:
        along = old[...] + per_frame(beta[0:1], VS) * way[...]
        volume[...] = vol[...] + scale * along
    direction[...] = along
    residual[...] = res[...] - scale[:, :RO] * image[...]
    step[...] = wide(alpha)


def forward_body(here, near, far, back, dense, out, field):
    row = jnp.zeros((1, LANES), F32)
    for j, part in enumerate((here, back, far, near)):
        field[:, j * VS : (j + 1) * VS] = part[:FH]
        row = row + row_of(part[FH:])
    rows = as_rows(row, RO)
    for c in range(NC):
        out[c, FH:] = rows
    wide_part = 4 * RS
    for h in range(NK):
        for q in range(RAYS // wide_part):
            at = h * RAYS + q * wide_part
            part = lax.dot_general(
                field[...],
                dense[at : at + wide_part],
                (((1,), (1,)), ((), ())),
                preferred_element_type=F32,
            ).astype(BF)
            for c in range(4):
                out[q * 4 + c, :FH, h * RS : (h + 1) * RS] = part[:, c * RS : (c + 1) * RS]


def gathered(arrived):
    value = arrived[0].astype(F32)
    for c in range(1, NC):
        value = value + arrived[c].astype(F32)
    return value[:FH], jnp.sum(value[FH:, :LANES], axis=0, keepdims=True)


def image_first_body(arrived, res, last, image, gamma, guess, message):
    value, row = gathered(arrived)
    image[...] = value
    gamma[...] = wide(row)
    about = last[0:1] / row
    about = jnp.where((about > 0.0) & (about < jnp.inf), about, 1.0)
    guess[...] = wide(about)
    put_all(message, res[...] - per_frame(about, RO) * value, squares(value))


def image_next_body(arrived, res, about, previous, last, image, gamma, beta, message):
    value, row = gathered(arrived)
    ratio = row / last[0:1]
    value = value + per_frame(ratio, RO) * previous[...]
    image[...] = value
    gamma[...] = wide(row)
    beta[...] = wide(ratio)
    put_all(message, res[...] - per_frame(about[0:1], RO) * value, squares(value))


def image_last_body(arrived, previous, last, image, gamma, beta, norms):
    value, row = gathered(arrived)
    ratio = row / last[0:1]
    value = value + per_frame(ratio, RO) * previous[...]
    image[...] = value
    gamma[...] = wide(row)
    beta[...] = wide(ratio)
    norm = wide(squares(value))
    for c in range(NC):
        norms[c] = norm


def norm_body(arrived, norms):
    total = arrived[0]
    for c in range(1, NC):
        total = total + arrived[c]
    for x in range(NX):
        norms[x] = total


def final_body(k, norms, gamma, search, beta, way, vol, res, image, mine, other, volume):
    total = norms[0, 0:1]
    for x in range(1, NX):
        total = total + norms[x, 0:1]
    alpha = per_frame(gamma[0:1] / total, VS)
    along = search[...] + per_frame(beta[0:1], VS) * way[...]
    volume[...] = vol[...] + alpha * along
    residual = res[...] - alpha[:, :RO] * image[...]
    mine[:, :VH] = volume[:, pl.ds(pl.multiple_of(k[0] * VH, VH), VH)]
    other[:, :VH] = volume[:, pl.ds(pl.multiple_of((1 - k[0]) * VH, VH), VH)]
    mine[:, VH:] = residual[:, :RS]
    other[:, VH:] = residual[:, RS:]


def finish_body(k, mine, other, volume, residual, turned):
    turned[pl.ds(pl.multiple_of(k[0] * FH, FH), FH)] = mine[...]
    turned[pl.ds(pl.multiple_of((1 - k[0]) * FH, FH), FH)] = other[...]
    whole = turned[...].T
    volume[...] = whole[:VH]
    residual[...] = whole[VH:]


def shifted(value, axis, by):
    n = lax.axis_size(axis)
    return lax.ppermute(value, axis, [(i, (i + by) % n) for i in range(n)])


def exchanged(parts, axis):
    return lax.all_to_all(parts, axis, split_axis=0, concat_axis=0, tiled=True)


LINE = (8, LANES)
COLUMN = (NC, FH + PAD, RO)
SHARD = (FH + PAD, VS)


def local(tiles, tile_row, tile_col, tile_count, sinogram):
    x = lax.axis_index("x").astype(jnp.int32).reshape(1)
    k = lax.axis_index("k").astype(jnp.int32).reshape(1)
    line = shape(LINE, F32)
    rays = shape((FH, RO), F32)
    voxels = shape((FH, VS), F32)
    column = shape(COLUMN, BF)
    shard = shape(SHARD, BF)

    table = jnp.concatenate(
        [tile_row[0], tile_col[0], jnp.broadcast_to(tile_count, tile_row.shape[1:])], axis=0
    )
    stored = tiles[0, 0]
    stored2 = shifted(stored, "k", 1)
    table2 = shifted(table, "k", 1)
    half = shape((FH, RS), F32)
    mine, other = kernel(
        turn_body, "turn", (half, half), (k, sinogram[0]), (pltpu.VMEM((FRAMES, RS), F32),)
    )
    residual, message = kernel(
        start_body, "start", (rays, column), (mine, shifted(other, "k", 1))
    )
    arrived = exchanged(message, COL)
    dense = build(x, table, table2, stored, stored2, arrived)

    def backward(arrived):
        own, norm, *pieces = kernel(
            backward_body,
            "backward",
            (voxels, line, shard, shard, shard),
            (arrived, dense),
            (pltpu.VMEM((FH, NK * RAYS), BF),),
            24,
        )
        far = shifted(pieces[1], "x", 2)
        near = shifted(pieces[0], "x", 1)
        back = shifted(pieces[2], "x", 3)
        return own, norm, near, far, back

    def forward(message):
        far = shifted(message, "x", 2)
        near = shifted(message, "x", 1)
        back = shifted(message, "x", 3)
        out = kernel(
            forward_body,
            "forward",
            column,
            (message, near, far, back, dense),
            (pltpu.VMEM((FH, VOX), BF),),
            24,
        )
        return exchanged(out, COL)

    search, shard_out, last = kernel(first_body, "first", (voxels, shard, line), backward(arrived))
    image, gamma, guess, message = kernel(
        image_first_body,
        "image_first",
        (rays, line, line, column),
        (forward(shard_out), residual, last),
    )
    beta = direction = volume = None
    for step in range(1, ITERS):
        state = (search, residual, image, gamma, guess)
        if step > 1:
            state += (beta, direction, volume)

        def body(*refs, first=step == 1):
            next_body(first, *refs)

        search, direction, volume, residual, shard_out, guess = kernel(
            body,
            "next",
            (voxels, voxels, voxels, rays, shard, line),
            (*backward(exchanged(message, COL)), *state),
        )
        arrived = forward(shard_out)
        if step + 1 < ITERS:
            image, gamma, beta, message = kernel(
                image_next_body,
                "image_next",
                (rays, line, line, column),
                (arrived, residual, guess, image, gamma),
            )
    image, gamma, beta, norms = kernel(
        image_last_body,
        "image_last",
        (rays, line, line, shape((NC, *LINE), F32)),
        (arrived, image, gamma),
    )
    norms = kernel(norm_body, "norm", shape((NX, *LINE), F32), (exchanged(norms, COL),))
    both = shape((FH, VH + RS), F32)
    mine, other = kernel(
        final_body,
        "final",
        (both, both),
        (k, exchanged(norms, "x"), gamma, search, beta, direction, volume, residual, image),
        (pltpu.VMEM((FH, VS), F32),),
    )
    volume, residual = kernel(
        finish_body,
        "finish",
        (shape((VH, FRAMES), F32), shape((RS, FRAMES), F32)),
        (k, mine, shifted(other, "k", 1)),
        (pltpu.VMEM((FRAMES, VH + RS), F32),),
    )
    return volume[None], residual[None]


def solution(mesh):
    finer = Mesh(mesh.devices.reshape(4, 2, 4, 4), ("x", "k", "y", "z"))
    placed = (
        P(ROW, COL, None, None, None),
        P(ROW, COL, None),
        P(ROW, COL, None),
        P(ROW, COL),
        P(ROW, COL, None),
    )
    return jax.shard_map(
        local,
        mesh=finer,
        in_specs=placed,
        out_specs=(P(COL, ROW, None), P(ROW, COL, None)),
        check_vma=False,
    )
```

```python
import functools

import jax
import jax.numpy as jnp
from jax import lax
from jax.experimental import pallas as pl
from jax.experimental.pallas import tpu as pltpu
from jax.sharding import Mesh
from jax.sharding import PartitionSpec as P

ROW = ("x", "k")
COL = ("y", "z")
NX, NK, NC = 4, 2, 16
TILE = 128
RAYS = 2048
VOX = 2048
FRAMES = 128
ITERS = 4
FH = FRAMES // NK
RS = RAYS // NC
RO = NK * RS
VS = VOX // NX
VH = VS // NK
PAD = 8
LANES = 128
BF = jnp.bfloat16
F32 = jnp.float32


def vmem():
    return pl.BlockSpec(memory_space=pltpu.VMEM)


def smem():
    return pl.BlockSpec(memory_space=pltpu.SMEM)


def hbm():
    return pl.BlockSpec(memory_space=pltpu.HBM)


def shape(dims, dtype):
    return jax.ShapeDtypeStruct(dims, dtype)


def kernel(body, name, outs, ins, scratch=(), limit=4):
    return pl.pallas_call(
        body,
        name=name,
        out_shape=outs,
        in_specs=[smem() if a.dtype == jnp.int32 else vmem() for a in ins],
        out_specs=jax.tree.map(lambda _: vmem(), outs),
        scratch_shapes=list(scratch),
        compiler_params=pltpu.CompilerParams(vmem_limit_bytes=limit << 20),
    )(*ins)


def squares(values):
    total = values[:, :LANES] * values[:, :LANES]
    for i in range(LANES, values.shape[1], LANES):
        total += values[:, i : i + LANES] * values[:, i : i + LANES]
    square = jnp.concatenate([total, jnp.zeros((LANES - FH, LANES), F32)], axis=0)
    return jnp.sum(square.T, axis=0, keepdims=True)


def per_frame(row, width):
    column = jnp.broadcast_to(row, (LANES, LANES)).T[:FH]
    return jnp.concatenate([column] * (width // LANES), axis=1)


def as_rows(row, width):
    high = row.astype(BF).astype(F32)
    rest = row - high
    mid = rest.astype(BF).astype(F32)
    low = rest - mid
    i = lax.broadcasted_iota(jnp.int32, (PAD, LANES), 0)
    zero = jnp.zeros((PAD, LANES), F32)
    rows = jnp.where(i == 0, high, jnp.where(i == 1, mid, jnp.where(i == 2, low, zero)))
    return jnp.concatenate([rows, jnp.zeros((PAD, width - LANES), F32)], axis=1).astype(BF)


def row_of(rows):
    return jnp.sum(rows[:, :LANES].astype(F32), axis=0, keepdims=True)


def wide(row):
    return jnp.broadcast_to(row, (8, LANES))


def put(message, values, row):
    message[:FH] = values.astype(BF)
    message[FH:] = as_rows(row, message.shape[1])


def put_all(message, values, row):
    part = values.astype(BF)
    rows = as_rows(row, RO)
    for c in range(NC):
        message[c, :FH] = part
        message[c, FH:] = rows


def turn_body(k, sino, mine, other, turned):
    turned[...] = sino[...].T
    mine[...] = turned[pl.ds(pl.multiple_of(k[0] * FH, FH), FH)]
    other[...] = turned[pl.ds(pl.multiple_of((1 - k[0]) * FH, FH), FH)]


def start_body(mine, other, residual, message):
    values = jnp.concatenate([mine[...], other[...]], axis=1)
    residual[...] = values
    put_all(message, values, squares(values))


def build_body(x, table, table2, tiles, tiles2, after, dense, sem):
    dense[...] = jnp.zeros_like(dense)
    shift = x[0] * (NC // NX)

    def copy(half, t):
        index, stored = ((table, tiles), (table2, tiles2))[half]
        r = pl.multiple_of(index[0, t] * TILE + half * RAYS, TILE)
        c = pl.multiple_of((index[1, t] + NC - shift) % NC * TILE, TILE)
        return pltpu.make_async_copy(stored.at[t], dense.at[pl.ds(r, TILE), pl.ds(c, TILE)], sem)

    def start(half):
        def step(t, carry):
            copy(half, t).start()
            return carry

        return step

    def wait(half):
        def step(t, carry):
            copy(half, t).wait()
            return carry

        return step

    lax.fori_loop(0, table[2, 0], start(0), 0)
    lax.fori_loop(0, table2[2, 0], start(1), 0)
    lax.fori_loop(0, table[2, 0], wait(0), 0)
    lax.fori_loop(0, table2[2, 0], wait(1), 0)


def build(x, table, table2, tiles, tiles2, after):
    return pl.pallas_call(
        build_body,
        name="build",
        out_shape=pltpu.VMEM((NK * RAYS, VOX), BF),
        in_specs=[smem(), smem(), smem(), hbm(), hbm(), vmem()],
        out_specs=vmem(),
        scratch_shapes=[pltpu.SemaphoreType.DMA(())],
        compiler_params=pltpu.CompilerParams(vmem_limit_bytes=4 << 20),
    )(x, table, table2, tiles, tiles2, after)


def gather_body(arrived, dense, field, norm, far):
    seen = arrived[0, FH:].astype(F32)
    for c in range(NC):
        part = arrived[c, :FH]
        for h in range(NK):
            field[:, h * RAYS + c * RS : h * RAYS + (c + 1) * RS] = part[:, h * RS : (h + 1) * RS]
        if c:
            seen += arrived[c, FH:].astype(F32)
    row = row_of(seen)
    norm[...] = wide(row)
    part = jnp.dot(field[...], dense[:, 2 * VS : 3 * VS], preferred_element_type=F32)
    put(far, part, row)


def piece_body(j, field, norm, dense, out):
    part = jnp.dot(field[...], dense[:, j * VS : (j + 1) * VS], preferred_element_type=F32)
    if j:
        put(out, part, norm[0:1])
    else:
        out[...] = part


def arrived_sum(own, norm, pieces):
    value = own[...]
    row = norm[0:1]
    for p in pieces:
        value = value + p[:FH].astype(F32)
        row = row + row_of(p[FH:])
    return value, row


def first_body(own, norm, p1, p2, p3, search, message, total):
    value, row = arrived_sum(own, norm, (p1, p2, p3))
    search[...] = value
    put(message, value, squares(value))
    total[...] = wide(row)


def next_body(first, own, norm, p1, p2, p3, *refs):
    if first:
        old, res, image, gamma, guess = refs[:5]
        outs = refs[5:]
    else:
        old, res, image, gamma, guess, beta, way, vol = refs[:8]
        outs = refs[8:]
    search, direction, volume, residual, message, step = outs
    value, row = arrived_sum(own, norm, (p1, p2, p3))
    alpha = gamma[0:1] / row
    ratio = per_frame(alpha / guess[0:1], VS)
    fresh = (1.0 - ratio) * old[...] + ratio * value
    search[...] = fresh
    put(message, fresh, squares(fresh))
    scale = per_frame(alpha, VS)
    if first:
        along = old[...]
        volume[...] = scale * along
    else:
        along = old[...] + per_frame(beta[0:1], VS) * way[...]
        volume[...] = vol[...] + scale * along
    direction[...] = along
    residual[...] = res[...] - scale[:, :RO] * image[...]
    step[...] = wide(alpha)


def part_of(j, message, dense, at, size):
    return lax.dot_general(
        message[:FH],
        dense[at : at + size, j * VS : (j + 1) * VS],
        (((1,), (1,)), ((), ())),
        preferred_element_type=F32,
    )


def part_body(j, message, dense, *refs):
    image = refs[-1]
    size = 4 * RS
    for at in range(0, NK * RAYS, size):
        part = part_of(j, message, dense, at, size)
        if len(refs) > 1:
            part = part + refs[0][:, at : at + size]
        image[:, at : at + size] = part


def forward_body(j, message, dense, so_far, m1, m2, m3, out):
    row = jnp.zeros((1, LANES), F32)
    for m in (message, m1, m2, m3):
        row = row + row_of(m[FH:])
    rows = as_rows(row, RO)
    for c in range(NC):
        out[c, FH:] = rows
    size = 4 * RS
    for at in range(0, NK * RAYS, size):
        part = part_of(j, message, dense, at, size) + so_far[:, at : at + size]
        part = part.astype(BF)
        h, first = at // RAYS, at % RAYS // RS
        for c in range(4):
            out[first + c, :FH, h * RS : (h + 1) * RS] = part[:, c * RS : (c + 1) * RS]


def gathered(arrived):
    value = arrived[0].astype(F32)
    for c in range(1, NC):
        value = value + arrived[c].astype(F32)
    return value[:FH], jnp.sum(value[FH:, :LANES], axis=0, keepdims=True)


def image_first_body(arrived, res, last, image, gamma, guess, message):
    value, row = gathered(arrived)
    image[...] = value
    gamma[...] = wide(row)
    about = last[0:1] / row
    about = jnp.where((about > 0.0) & (about < jnp.inf), about, 1.0)
    guess[...] = wide(about)
    put_all(message, res[...] - per_frame(about, RO) * value, squares(value))


def image_next_body(arrived, res, about, previous, last, image, gamma, beta, message):
    value, row = gathered(arrived)
    ratio = row / last[0:1]
    value = value + per_frame(ratio, RO) * previous[...]
    image[...] = value
    gamma[...] = wide(row)
    beta[...] = wide(ratio)
    put_all(message, res[...] - per_frame(about[0:1], RO) * value, squares(value))


def image_last_body(arrived, previous, last, image, gamma, beta, norms):
    value, row = gathered(arrived)
    ratio = row / last[0:1]
    value = value + per_frame(ratio, RO) * previous[...]
    image[...] = value
    gamma[...] = wide(row)
    beta[...] = wide(ratio)
    norms[...] = wide(squares(value))


def pair_body(mine, other, norm):
    norm[...] = mine[...] + other[...]


def pairs_body(mine, other, norms):
    for c in range(NC):
        norms[c] = mine[...] + other[...]


def final_body(k, norms, gamma, search, beta, way, vol, res, image, mine, other, volume):
    total = norms[0, 0:1]
    for c in range(1, NC):
        total = total + norms[c, 0:1]
    alpha = per_frame(gamma[0:1] / total, VS)
    along = search[...] + per_frame(beta[0:1], VS) * way[...]
    volume[...] = vol[...] + alpha * along
    residual = res[...] - alpha[:, :RO] * image[...]
    mine[:, :VH] = volume[:, pl.ds(pl.multiple_of(k[0] * VH, VH), VH)]
    other[:, :VH] = volume[:, pl.ds(pl.multiple_of((1 - k[0]) * VH, VH), VH)]
    mine[:, VH:] = residual[:, :RS]
    other[:, VH:] = residual[:, RS:]


def finish_body(k, mine, other, volume, residual, turned):
    turned[pl.ds(pl.multiple_of(k[0] * FH, FH), FH)] = mine[...]
    turned[pl.ds(pl.multiple_of((1 - k[0]) * FH, FH), FH)] = other[...]
    whole = turned[...].T
    volume[...] = whole[:VH]
    residual[...] = whole[VH:]


def shifted(value, axis, by):
    n = lax.axis_size(axis)
    return lax.ppermute(value, axis, [(i, (i + by) % n) for i in range(n)])


def swapped(value, pairs):
    return lax.ppermute(value, "x", [(i, j) for a, b in pairs for i, j in ((a, b), (b, a))])


def exchanged(parts, axis):
    return lax.all_to_all(parts, axis, split_axis=0, concat_axis=0, tiled=True)


LINE = (8, LANES)
COLUMN = (NC, FH + PAD, RO)
SHARD = (FH + PAD, VS)


def local(tiles, tile_row, tile_col, tile_count, sinogram):
    x = lax.axis_index("x").astype(jnp.int32).reshape(1)
    k = lax.axis_index("k").astype(jnp.int32).reshape(1)
    line = shape(LINE, F32)
    rays = shape((FH, RO), F32)
    voxels = shape((FH, VS), F32)
    column = shape(COLUMN, BF)
    shard = shape(SHARD, BF)

    table = jnp.concatenate(
        [tile_row[0], tile_col[0], jnp.broadcast_to(tile_count, tile_row.shape[1:])], axis=0
    )
    half = shape((FH, RS), F32)
    mine, other = kernel(
        turn_body, "turn", (half, half), (k, sinogram[0]), (pltpu.VMEM((FRAMES, RS), F32),)
    )
    table2 = shifted(table, "k", 1)
    other = shifted(other, "k", 1)
    stored, other, table2, x = lax.optimization_barrier((tiles[0, 0], other, table2, x))
    stored2 = shifted(stored, "k", 1)
    residual, message = kernel(start_body, "start", (rays, column), (mine, other))
    arrived = exchanged(message, COL)
    dense = build(x, table, table2, stored, stored2, arrived)

    def backward(arrived):
        field, norm, p2 = kernel(
            gather_body, "gather", (shape((FH, NK * RAYS), BF), line, shard), (arrived, dense), limit=16
        )

        def piece(j, out):
            return kernel(
                functools.partial(piece_body, j), f"piece{j}", out, (field, norm, dense), limit=16
            )

        far = shifted(p2, "x", 2)
        near = shifted(piece(1, shard), "x", 1)
        back = shifted(piece(3, shard), "x", 3)
        return piece(0, voxels), norm, near, back, far

    def forward(message):
        far = shifted(message, "x", 2)
        near = shifted(message, "x", 1)
        back = shifted(message, "x", 3)
        image = ()
        for j, part in ((0, message), (3, near), (1, back)):
            image = (
                kernel(
                    functools.partial(part_body, j),
                    f"part{j}",
                    shape((FH, NK * RAYS), F32),
                    (part, dense, *image),
                    limit=16,
                ),
            )
        out = kernel(
            functools.partial(forward_body, 2),
            "forward",
            column,
            (far, dense, *image, message, near, back),
            limit=16,
        )
        return exchanged(out, COL)

    search, shard_out, last = kernel(first_body, "first", (voxels, shard, line), backward(arrived))
    image, gamma, guess, message = kernel(
        image_first_body,
        "image_first",
        (rays, line, line, column),
        (forward(shard_out), residual, last),
    )
    beta = direction = volume = None
    for step in range(1, ITERS):
        state = (search, residual, image, gamma, guess)
        if step > 1:
            state += (beta, direction, volume)

        def body(*refs, first=step == 1):
            next_body(first, *refs)

        search, direction, volume, residual, shard_out, guess = kernel(
            body,
            "next",
            (voxels, voxels, voxels, rays, shard, line),
            (*backward(exchanged(message, COL)), *state),
        )
        arrived = forward(shard_out)
        if step + 1 < ITERS:
            image, gamma, beta, message = kernel(
                image_next_body,
                "image_next",
                (rays, line, line, column),
                (arrived, residual, guess, image, gamma),
            )
    image, gamma, beta, norm = kernel(
        image_last_body,
        "image_last",
        (rays, line, line, line),
        (arrived, image, gamma),
    )
    norm = kernel(pair_body, "pair", line, (norm, swapped(norm, ((0, 1), (2, 3)))))
    norms = kernel(
        pairs_body, "pairs", shape((NC, *LINE), F32), (norm, swapped(norm, ((1, 2), (3, 0))))
    )
    both = shape((FH, VH + RS), F32)
    mine, other = kernel(
        final_body,
        "final",
        (both, both),
        (k, exchanged(norms, COL), gamma, search, beta, direction, volume, residual, image),
        (pltpu.VMEM((FH, VS), F32),),
    )
    volume, residual = kernel(
        finish_body,
        "finish",
        (shape((VH, FRAMES), F32), shape((RS, FRAMES), F32)),
        (k, mine, shifted(other, "k", 1)),
        (pltpu.VMEM((FRAMES, VH + RS), F32),),
    )
    return volume[None], residual[None]


def solution(mesh):
    finer = Mesh(mesh.devices.reshape(4, 2, 4, 4), ("x", "k", "y", "z"))
    placed = (
        P(ROW, COL, None, None, None),
        P(ROW, COL, None),
        P(ROW, COL, None),
        P(ROW, COL),
        P(ROW, COL, None),
    )
    return jax.shard_map(
        local,
        mesh=finer,
        in_specs=placed,
        out_specs=(P(COL, ROW, None), P(ROW, COL, None)),
        check_vma=False,
    )
```

```python
import functools

import jax
import jax.numpy as jnp
from jax import lax
from jax.experimental import pallas as pl
from jax.experimental.pallas import tpu as pltpu
from jax.sharding import Mesh
from jax.sharding import PartitionSpec as P

ROW = ("x", "k")
COL = ("y", "z")
NX, NK, NC = 4, 2, 16
TILE = 128
RAYS = 2048
VOX = 2048
FRAMES = 128
ITERS = 4
FH = FRAMES // NK
RS = RAYS // NC
RO = NK * RS
VS = VOX // NX
VH = VS // NK
PAD = 8
LANES = 128
BF = jnp.bfloat16
F32 = jnp.float32


def vmem():
    return pl.BlockSpec(memory_space=pltpu.VMEM)


def smem():
    return pl.BlockSpec(memory_space=pltpu.SMEM)


def hbm():
    return pl.BlockSpec(memory_space=pltpu.HBM)


def shape(dims, dtype):
    return jax.ShapeDtypeStruct(dims, dtype)


def kernel(body, name, outs, ins, scratch=(), limit=4):
    return pl.pallas_call(
        body,
        name=name,
        out_shape=outs,
        in_specs=[smem() if a.dtype == jnp.int32 else vmem() for a in ins],
        out_specs=jax.tree.map(lambda _: vmem(), outs),
        scratch_shapes=list(scratch),
        compiler_params=pltpu.CompilerParams(vmem_limit_bytes=limit << 20),
    )(*ins)


def squares(values):
    total = values[:, :LANES] * values[:, :LANES]
    for i in range(LANES, values.shape[1], LANES):
        total += values[:, i : i + LANES] * values[:, i : i + LANES]
    square = jnp.concatenate([total, jnp.zeros((LANES - FH, LANES), F32)], axis=0)
    return jnp.sum(square.T, axis=0, keepdims=True)


def per_frame(row, width):
    column = jnp.broadcast_to(row, (LANES, LANES)).T[:FH]
    return jnp.concatenate([column] * (width // LANES), axis=1)


def as_rows(row, width):
    high = row.astype(BF).astype(F32)
    rest = row - high
    mid = rest.astype(BF).astype(F32)
    low = rest - mid
    i = lax.broadcasted_iota(jnp.int32, (PAD, LANES), 0)
    zero = jnp.zeros((PAD, LANES), F32)
    rows = jnp.where(i == 0, high, jnp.where(i == 1, mid, jnp.where(i == 2, low, zero)))
    return jnp.concatenate([rows, jnp.zeros((PAD, width - LANES), F32)], axis=1).astype(BF)


def row_of(rows):
    return jnp.sum(rows[:, :LANES].astype(F32), axis=0, keepdims=True)


def wide(row):
    return jnp.broadcast_to(row, (8, LANES))


def put(message, values, row):
    message[:FH] = values.astype(BF)
    message[FH:] = as_rows(row, message.shape[1])


def put_all(message, values, row):
    part = values.astype(BF)
    rows = as_rows(row, RO)
    for c in range(NC):
        message[c, :FH] = part
        message[c, FH:] = rows


def turn_body(k, sino, mine, other, turned):
    turned[...] = sino[...].T
    mine[...] = turned[pl.ds(pl.multiple_of(k[0] * FH, FH), FH)]
    other[...] = turned[pl.ds(pl.multiple_of((1 - k[0]) * FH, FH), FH)]


def start_body(mine, other, residual, message):
    values = jnp.concatenate([mine[...], other[...]], axis=1)
    residual[...] = values
    put_all(message, values, squares(values))


def build_body(x, table, table2, tiles, tiles2, after, dense, sem):
    dense[...] = jnp.zeros_like(dense)
    shift = x[0] * (NC // NX)

    def copy(half, t):
        index, stored = ((table, tiles), (table2, tiles2))[half]
        r = pl.multiple_of(index[0, t] * TILE + half * RAYS, TILE)
        c = pl.multiple_of((index[1, t] + NC - shift) % NC * TILE, TILE)
        return pltpu.make_async_copy(stored.at[t], dense.at[pl.ds(r, TILE), pl.ds(c, TILE)], sem)

    def start(half):
        def step(t, carry):
            copy(half, t).start()
            return carry

        return step

    def wait(half):
        def step(t, carry):
            copy(half, t).wait()
            return carry

        return step

    lax.fori_loop(0, table[2, 0], start(0), 0)
    lax.fori_loop(0, table2[2, 0], start(1), 0)
    lax.fori_loop(0, table[2, 0], wait(0), 0)
    lax.fori_loop(0, table2[2, 0], wait(1), 0)


def build(x, table, table2, tiles, tiles2, after):
    return pl.pallas_call(
        build_body,
        name="build",
        out_shape=pltpu.VMEM((NK * RAYS, VOX), BF),
        in_specs=[smem(), smem(), smem(), hbm(), hbm(), vmem()],
        out_specs=vmem(),
        scratch_shapes=[pltpu.SemaphoreType.DMA(())],
        compiler_params=pltpu.CompilerParams(vmem_limit_bytes=4 << 20),
    )(x, table, table2, tiles, tiles2, after)


def piece_of(j, field, dense, put_part):
    half = VS // 2

    def step(i, carry):
        at = pl.multiple_of(j * VS + i * half, half)
        here = pl.ds(pl.multiple_of(i * half, half), half)
        put_part(here, jnp.dot(field[...], dense[:, pl.ds(at, half)], preferred_element_type=F32))
        return carry

    lax.fori_loop(0, 2, step, 0)


def gather_body(arrived, dense, field, norm, far):
    seen = arrived[0, FH:].astype(F32)
    for c in range(NC):
        part = arrived[c, :FH]
        for h in range(NK):
            field[:, h * RAYS + c * RS : h * RAYS + (c + 1) * RS] = part[:, h * RS : (h + 1) * RS]
        if c:
            seen += arrived[c, FH:].astype(F32)
    row = row_of(seen)
    norm[...] = wide(row)
    far[FH:] = as_rows(row, VS)

    def put_part(here, part):
        far[:FH, here] = part.astype(BF)

    piece_of(2, field, dense, put_part)


def own_body(field, dense, own):
    def put_part(here, part):
        own[:, here] = part

    piece_of(0, field, dense, put_part)


def back_body(field, norm, dense, back):
    back[FH:] = as_rows(norm[0:1], VS)

    def put_part(here, part):
        back[:FH, here] = part.astype(BF)

    piece_of(3, field, dense, put_part)


def near_body(passed, field, norm, dense, near):
    near[FH:] = as_rows(norm[0:1] + row_of(passed[FH:]), VS)

    def put_part(here, part):
        near[:FH, here] = (part + passed[:FH, here].astype(F32)).astype(BF)

    piece_of(1, field, dense, put_part)


def arrived_sum(own, norm, pieces):
    value = own[...]
    row = norm[0:1]
    for p in pieces:
        value = value + p[:FH].astype(F32)
        row = row + row_of(p[FH:])
    return value, row


def first_body(own, norm, p1, p2, search, message, total):
    value, row = arrived_sum(own, norm, (p1, p2))
    search[...] = value
    put(message, value, squares(value))
    total[...] = wide(row)


def next_body(first, own, norm, p1, p2, *refs):
    if first:
        old, res, image, gamma, guess = refs[:5]
        outs = refs[5:]
    else:
        old, res, image, gamma, guess, beta, way, vol = refs[:8]
        outs = refs[8:]
    search, direction, volume, residual, message, step = outs
    value, row = arrived_sum(own, norm, (p1, p2))
    alpha = gamma[0:1] / row
    ratio = per_frame(alpha / guess[0:1], VS)
    fresh = (1.0 - ratio) * old[...] + ratio * value
    search[...] = fresh
    put(message, fresh, squares(fresh))
    scale = per_frame(alpha, VS)
    if first:
        along = old[...]
        volume[...] = scale * along
    else:
        along = old[...] + per_frame(beta[0:1], VS) * way[...]
        volume[...] = vol[...] + scale * along
    direction[...] = along
    residual[...] = res[...] - scale[:, :RO] * image[...]
    step[...] = wide(alpha)


def part_of(places, messages, dense, put_part):
    size = 4 * RS
    for h in range(NK):

        def step(i, carry, h=h):
            at = pl.multiple_of(h * RAYS + i * size, size)
            total = None
            for j, m in zip(places, messages):
                part = lax.dot_general(
                    m[:FH],
                    dense[pl.ds(at, size), j * VS : (j + 1) * VS],
                    (((1,), (1,)), ((), ())),
                    preferred_element_type=F32,
                )
                total = part if total is None else total + part
            put_part(h, i, pl.ds(at, size), total)
            return carry

        lax.fori_loop(0, RAYS // size, step, 0)


def here_body(message, dense, image):
    def put_part(h, i, rays, part):
        image[:, rays] = part

    part_of((0,), (message,), dense, put_part)


def beside_body(near, back, dense, so_far, image):
    def put_part(h, i, rays, part):
        image[:, rays] = so_far[:, rays] + part

    part_of((3, 1), (near, back), dense, put_part)


def forward_body(far, dense, so_far, here, near, back, out):
    row = jnp.zeros((1, LANES), F32)
    for m in (here, near, back, far):
        row = row + row_of(m[FH:])
    rows = as_rows(row, RO)
    for c in range(NC):
        out[c, FH:] = rows

    def put_part(h, i, rays, part):
        part = (so_far[:, rays] + part).astype(BF)
        for c in range(4):
            out[i * 4 + c, :FH, h * RS : (h + 1) * RS] = part[:, c * RS : (c + 1) * RS]

    part_of((2,), (far,), dense, put_part)


def gathered(arrived):
    value = arrived[0].astype(F32)
    for c in range(1, NC):
        value = value + arrived[c].astype(F32)
    return value[:FH], jnp.sum(value[FH:, :LANES], axis=0, keepdims=True)


def image_first_body(arrived, res, last, image, gamma, guess, message):
    value, row = gathered(arrived)
    image[...] = value
    gamma[...] = wide(row)
    about = last[0:1] / row
    about = jnp.where((about > 0.0) & (about < jnp.inf), about, 1.0)
    guess[...] = wide(about)
    put_all(message, res[...] - per_frame(about, RO) * value, squares(value))


def image_next_body(arrived, res, about, previous, last, image, gamma, beta, message):
    value, row = gathered(arrived)
    ratio = row / last[0:1]
    value = value + per_frame(ratio, RO) * previous[...]
    image[...] = value
    gamma[...] = wide(row)
    beta[...] = wide(ratio)
    put_all(message, res[...] - per_frame(about[0:1], RO) * value, squares(value))


def image_last_body(arrived, previous, last, image, gamma, beta, norms):
    value, row = gathered(arrived)
    ratio = row / last[0:1]
    value = value + per_frame(ratio, RO) * previous[...]
    image[...] = value
    gamma[...] = wide(row)
    beta[...] = wide(ratio)
    norms[...] = wide(squares(value))


def pair_body(mine, other, norm):
    norm[...] = mine[...] + other[...]


def pairs_body(mine, other, norms):
    for c in range(NC):
        norms[c] = mine[...] + other[...]


def final_body(k, norms, gamma, search, beta, way, vol, res, image, mine, other, volume):
    total = norms[0, 0:1]
    for c in range(1, NC):
        total = total + norms[c, 0:1]
    alpha = per_frame(gamma[0:1] / total, VS)
    along = search[...] + per_frame(beta[0:1], VS) * way[...]
    volume[...] = vol[...] + alpha * along
    residual = res[...] - alpha[:, :RO] * image[...]
    mine[:, :VH] = volume[:, pl.ds(pl.multiple_of(k[0] * VH, VH), VH)]
    other[:, :VH] = volume[:, pl.ds(pl.multiple_of((1 - k[0]) * VH, VH), VH)]
    mine[:, VH:] = residual[:, :RS]
    other[:, VH:] = residual[:, RS:]


def finish_body(k, mine, other, volume, residual, turned):
    turned[pl.ds(pl.multiple_of(k[0] * FH, FH), FH)] = mine[...]
    turned[pl.ds(pl.multiple_of((1 - k[0]) * FH, FH), FH)] = other[...]
    whole = turned[...].T
    volume[...] = whole[:VH]
    residual[...] = whole[VH:]


def shifted(value, axis, by):
    n = lax.axis_size(axis)
    return lax.ppermute(value, axis, [(i, (i + by) % n) for i in range(n)])


def swapped(value, pairs):
    return lax.ppermute(value, "x", [(i, j) for a, b in pairs for i, j in ((a, b), (b, a))])


def exchanged(parts, axis):
    return lax.all_to_all(parts, axis, split_axis=0, concat_axis=0, tiled=True)


LINE = (8, LANES)
COLUMN = (NC, FH + PAD, RO)
SHARD = (FH + PAD, VS)


def local(tiles, tile_row, tile_col, tile_count, sinogram):
    x = lax.axis_index("x").astype(jnp.int32).reshape(1)
    k = lax.axis_index("k").astype(jnp.int32).reshape(1)
    line = shape(LINE, F32)
    rays = shape((FH, RO), F32)
    voxels = shape((FH, VS), F32)
    column = shape(COLUMN, BF)
    shard = shape(SHARD, BF)

    table = jnp.concatenate(
        [tile_row[0], tile_col[0], jnp.broadcast_to(tile_count, tile_row.shape[1:])], axis=0
    )
    half = shape((FH, RS), F32)
    mine, other = kernel(
        turn_body, "turn", (half, half), (k, sinogram[0]), (pltpu.VMEM((FRAMES, RS), F32),)
    )
    table2 = shifted(table, "k", 1)
    other = shifted(other, "k", 1)
    stored, other, table2, x = lax.optimization_barrier((tiles[0, 0], other, table2, x))
    stored2 = shifted(stored, "k", 1)
    residual, message = kernel(start_body, "start", (rays, column), (mine, other))
    arrived = exchanged(message, COL)
    dense = build(x, table, table2, stored, stored2, arrived)

    def backward(arrived):
        field, norm, far = kernel(
            gather_body, "gather", (shape((FH, NK * RAYS), BF), line, shard), (arrived, dense), limit=16
        )
        passed = shifted(far, "x", 1)
        back = shifted(kernel(back_body, "back", shard, (field, norm, dense), limit=16), "x", 3)
        near = shifted(
            kernel(near_body, "near", shard, (passed, field, norm, dense), limit=16), "x", 1
        )
        own = kernel(own_body, "own", voxels, (field, dense), limit=16)
        return own, norm, back, near

    def forward(message):
        near = shifted(message, "x", 1)
        back = shifted(message, "x", 3)
        rays2 = shape((FH, NK * RAYS), F32)
        image = kernel(here_body, "here", rays2, (message, dense), limit=16)
        near, image = lax.optimization_barrier((near, image))
        far = shifted(near, "x", 1)
        image = kernel(beside_body, "beside", rays2, (near, back, dense, image), limit=16)
        out = kernel(
            forward_body,
            "forward",
            column,
            (far, dense, image, message, near, back),
            limit=16,
        )
        return exchanged(out, COL)

    search, shard_out, last = kernel(first_body, "first", (voxels, shard, line), backward(arrived))
    image, gamma, guess, message = kernel(
        image_first_body,
        "image_first",
        (rays, line, line, column),
        (forward(shard_out), residual, last),
    )
    beta = direction = volume = None
    for step in range(1, ITERS):
        state = (search, residual, image, gamma, guess)
        if step > 1:
            state += (beta, direction, volume)

        def body(*refs, first=step == 1):
            next_body(first, *refs)

        search, direction, volume, residual, shard_out, guess = kernel(
            body,
            "next",
            (voxels, voxels, voxels, rays, shard, line),
            (*backward(exchanged(message, COL)), *state),
        )
        arrived = forward(shard_out)
        if step + 1 < ITERS:
            image, gamma, beta, message = kernel(
                image_next_body,
                "image_next",
                (rays, line, line, column),
                (arrived, residual, guess, image, gamma),
            )
    image, gamma, beta, norm = kernel(
        image_last_body,
        "image_last",
        (rays, line, line, line),
        (arrived, image, gamma),
    )
    norm = kernel(pair_body, "pair", line, (norm, swapped(norm, ((0, 1), (2, 3)))))
    norms = kernel(
        pairs_body, "pairs", shape((NC, *LINE), F32), (norm, swapped(norm, ((1, 2), (3, 0))))
    )
    both = shape((FH, VH + RS), F32)
    mine, other = kernel(
        final_body,
        "final",
        (both, both),
        (k, exchanged(norms, COL), gamma, search, beta, direction, volume, residual, image),
        (pltpu.VMEM((FH, VS), F32),),
    )
    volume, residual = kernel(
        finish_body,
        "finish",
        (shape((VH, FRAMES), F32), shape((RS, FRAMES), F32)),
        (k, mine, shifted(other, "k", 1)),
        (pltpu.VMEM((FRAMES, VH + RS), F32),),
    )
    return volume[None], residual[None]


def solution(mesh):
    finer = Mesh(mesh.devices.reshape(4, 2, 4, 4), ("x", "k", "y", "z"))
    placed = (
        P(ROW, COL, None, None, None),
        P(ROW, COL, None),
        P(ROW, COL, None),
        P(ROW, COL),
        P(ROW, COL, None),
    )
    return jax.shard_map(
        local,
        mesh=finer,
        in_specs=placed,
        out_specs=(P(COL, ROW, None), P(ROW, COL, None)),
        check_vma=False,
    )
```

```python
import functools

import jax
import jax.numpy as jnp
from jax import lax
from jax.experimental import pallas as pl
from jax.experimental.pallas import tpu as pltpu
from jax.sharding import Mesh
from jax.sharding import PartitionSpec as P

ROW = ("x", "k")
COL = ("y", "z")
NX, NK, NC = 4, 2, 16
TILE = 128
RAYS = 2048
VOX = 2048
FRAMES = 128
ITERS = 4
FH = FRAMES // NK
RS = RAYS // NC
RO = NK * RS
VS = VOX // NX
VH = VS // NK
VROWS = VS // 128 * FH
PAD = 8
LANES = 128
BF = jnp.bfloat16
F32 = jnp.float32


def vmem():
    return pl.BlockSpec(memory_space=pltpu.VMEM)


def smem():
    return pl.BlockSpec(memory_space=pltpu.SMEM)


def hbm():
    return pl.BlockSpec(memory_space=pltpu.HBM)


def shape(dims, dtype):
    return jax.ShapeDtypeStruct(dims, dtype)


def kernel(body, name, outs, ins, scratch=(), limit=4):
    return pl.pallas_call(
        body,
        name=name,
        out_shape=outs,
        in_specs=[smem() if a.dtype == jnp.int32 else vmem() for a in ins],
        out_specs=jax.tree.map(lambda _: vmem(), outs),
        scratch_shapes=list(scratch),
        compiler_params=pltpu.CompilerParams(vmem_limit_bytes=limit << 20),
    )(*ins)


def squares(values):
    total = values[:, :LANES] * values[:, :LANES]
    for i in range(LANES, values.shape[1], LANES):
        total += values[:, i : i + LANES] * values[:, i : i + LANES]
    square = jnp.concatenate([total, jnp.zeros((LANES - FH, LANES), F32)], axis=0)
    return jnp.sum(square.T, axis=0, keepdims=True)


def per_frame(row, width):
    column = jnp.broadcast_to(row, (LANES, LANES)).T[:FH]
    return jnp.concatenate([column] * (width // LANES), axis=1)


def as_rows(row):
    high = row.astype(BF).astype(F32)
    rest = row - high
    mid = rest.astype(BF).astype(F32)
    low = rest - mid
    i = lax.broadcasted_iota(jnp.int32, (PAD, LANES), 0)
    zero = jnp.zeros((PAD, LANES), F32)
    return jnp.where(i == 0, high, jnp.where(i == 1, mid, jnp.where(i == 2, low, zero))).astype(BF)


def row_of(rows):
    return jnp.sum(rows.astype(F32), axis=0, keepdims=True)


def wide(row):
    return jnp.broadcast_to(row, (8, LANES))


def stacked(values):
    return jnp.concatenate(
        [values[:, i : i + LANES] for i in range(0, values.shape[1], LANES)], axis=0
    )


def unstacked(rows):
    return jnp.concatenate([rows[i : i + FH] for i in range(0, rows.shape[0], FH)], axis=1)


def put(message, values, row):
    message[: message.shape[0] - PAD] = stacked(values.astype(BF))
    message[message.shape[0] - PAD :] = as_rows(row)


def put_all(message, values, row):
    part = stacked(values.astype(BF))
    rows = as_rows(row)
    for c in range(NC):
        message[c, : RO // LANES * FH] = part
        message[c, RO // LANES * FH :] = rows


def turn_body(k, sino, mine, other, turned):
    turned[...] = sino[...].T
    mine[...] = turned[pl.ds(pl.multiple_of(k[0] * FH, FH), FH)]
    other[...] = turned[pl.ds(pl.multiple_of((1 - k[0]) * FH, FH), FH)]


def start_body(mine, other, residual, message):
    values = jnp.concatenate([mine[...], other[...]], axis=1)
    residual[...] = values
    put_all(message, values, squares(values))


def build_body(x, table, table2, tiles, tiles2, after, dense, turned, sem, sem2):
    shift = x[0] * (NC // NX)
    halves = ((table, tiles, sem), (table2, tiles2, sem2))

    def copy(half, t):
        index, stored, done = halves[half]
        r = pl.multiple_of(index[0, t] * TILE + half * RAYS, TILE)
        c = pl.multiple_of((index[1, t] + NC - shift) % NC * TILE, TILE)
        return pltpu.make_async_copy(stored.at[t], dense.at[pl.ds(r, TILE), pl.ds(c, TILE)], done)

    for half in range(NK):

        def start(t, carry, half=half):
            copy(half, t).start()
            return carry

        dense[half * RAYS : (half + 1) * RAYS] = jnp.zeros((RAYS, VOX), BF)
        lax.fori_loop(0, halves[half][0][2, 0], start, 0)
    for half in range(NK):

        def wait(t, carry, half=half):
            copy(half, t).wait()
            return carry

        def turn(j, carry, half=half):
            voxels = pl.ds(pl.multiple_of(j * TILE, TILE), TILE)
            for i in range(half * RAYS, (half + 1) * RAYS, TILE):
                turned[voxels, i : i + TILE] = dense[i : i + TILE, voxels].T
            return carry

        lax.fori_loop(0, halves[half][0][2, 0], wait, 0)
        lax.fori_loop(0, VOX // TILE, turn, 0)


def build(x, table, table2, tiles, tiles2, after):
    return pl.pallas_call(
        build_body,
        name="build",
        out_shape=(pltpu.VMEM((NK * RAYS, VOX), BF), pltpu.VMEM((VOX, NK * RAYS), BF)),
        in_specs=[smem(), smem(), smem(), hbm(), hbm(), vmem()],
        out_specs=(vmem(), vmem()),
        scratch_shapes=[pltpu.SemaphoreType.DMA(()), pltpu.SemaphoreType.DMA(())],
        compiler_params=pltpu.CompilerParams(vmem_limit_bytes=4 << 20),
    )(x, table, table2, tiles, tiles2, after)


def gather_body(arrived, dense, field, norm, far):
    seen = arrived[0, NK * FH :].astype(F32)
    for c in range(NC):
        for h in range(NK):
            field[:, h * RAYS + c * RS : h * RAYS + (c + 1) * RS] = arrived[c, h * FH : (h + 1) * FH]
        if c:
            seen += arrived[c, NK * FH :].astype(F32)
    row = row_of(seen)
    norm[...] = wide(row)
    part = jnp.dot(field[...], dense[:, 2 * VS : 3 * VS], preferred_element_type=F32)
    put(far, part, row)


def piece_body(j, field, norm, dense, out):
    part = jnp.dot(field[...], dense[:, j * VS : (j + 1) * VS], preferred_element_type=F32)
    if j:
        put(out, part, norm[0:1])
    else:
        out[...] = part


def arrived_sum(own, norm, pieces):
    value = own[...]
    row = norm[0:1]
    for p in pieces:
        value = value + unstacked(p[:VROWS].astype(F32))
        row = row + row_of(p[VROWS:])
    return value, row


def first_body(own, norm, p1, p2, p3, search, message, total):
    value, row = arrived_sum(own, norm, (p1, p2, p3))
    search[...] = value
    put(message, value, squares(value))
    total[...] = wide(row)


def next_body(first, own, norm, p1, p2, p3, *refs):
    if first:
        old, res, image, gamma, guess = refs[:5]
        outs = refs[5:]
    else:
        old, res, image, gamma, guess, beta, way, vol = refs[:8]
        outs = refs[8:]
    search, direction, volume, residual, message, step = outs
    value, row = arrived_sum(own, norm, (p1, p2, p3))
    alpha = gamma[0:1] / row
    ratio = per_frame(alpha / guess[0:1], VS)
    fresh = (1.0 - ratio) * old[...] + ratio * value
    search[...] = fresh
    put(message, fresh, squares(fresh))
    scale = per_frame(alpha, VS)
    if first:
        along = old[...]
        volume[...] = scale * along
    else:
        along = old[...] + per_frame(beta[0:1], VS) * way[...]
        volume[...] = vol[...] + scale * along
    direction[...] = along
    residual[...] = res[...] - scale[:, :RO] * image[...]
    step[...] = wide(alpha)


SIZE = 4 * RS


def part_of(places, messages, turned, at):
    total = None
    for j, m in zip(places, messages):
        part = jnp.dot(
            unstacked(m[:VROWS]),
            turned[j * VS : (j + 1) * VS, at : at + SIZE],
            preferred_element_type=F32,
        )
        total = part if total is None else total + part
    return total


def here_body(here, turned, image):
    for at in range(0, NK * RAYS, SIZE):
        image[:, at : at + SIZE] = part_of((0,), (here,), turned, at)


def beside_body(near, back, turned, so_far, image):
    for at in range(0, NK * RAYS, SIZE):
        part = part_of((3, 1), (near, back), turned, at)
        image[:, at : at + SIZE] = so_far[:, at : at + SIZE] + part


def forward_body(far, turned, so_far, here, near, back, out):
    row = jnp.zeros((1, LANES), F32)
    for m in (here, near, back, far):
        row = row + row_of(m[VROWS:])
    rows = as_rows(row)
    for c in range(NC):
        out[c, NK * FH :] = rows
    for at in range(0, NK * RAYS, SIZE):
        part = (part_of((2,), (far,), turned, at) + so_far[:, at : at + SIZE]).astype(BF)
        h, first = at // RAYS, at % RAYS // RS
        for c in range(SIZE // RS):
            out[first + c, h * FH : (h + 1) * FH] = part[:, c * RS : (c + 1) * RS]


def gathered(arrived):
    value = arrived[0].astype(F32)
    for c in range(1, NC):
        value = value + arrived[c].astype(F32)
    return unstacked(value[: NK * FH]), jnp.sum(value[NK * FH :], axis=0, keepdims=True)


def image_first_body(arrived, res, last, image, gamma, guess, message):
    value, row = gathered(arrived)
    image[...] = value
    gamma[...] = wide(row)
    about = last[0:1] / row
    about = jnp.where((about > 0.0) & (about < jnp.inf), about, 1.0)
    guess[...] = wide(about)
    put_all(message, res[...] - per_frame(about, RO) * value, squares(value))


def image_next_body(arrived, res, about, previous, last, image, gamma, beta, message):
    value, row = gathered(arrived)
    ratio = row / last[0:1]
    value = value + per_frame(ratio, RO) * previous[...]
    image[...] = value
    gamma[...] = wide(row)
    beta[...] = wide(ratio)
    put_all(message, res[...] - per_frame(about[0:1], RO) * value, squares(value))


def image_last_body(arrived, previous, last, image, gamma, beta, norms):
    value, row = gathered(arrived)
    ratio = row / last[0:1]
    value = value + per_frame(ratio, RO) * previous[...]
    image[...] = value
    gamma[...] = wide(row)
    beta[...] = wide(ratio)
    norms[...] = wide(squares(value))


def pair_body(mine, other, norm):
    norm[...] = mine[...] + other[...]


def pairs_body(mine, other, norms):
    for c in range(NC):
        norms[c] = mine[...] + other[...]


def final_body(k, norms, gamma, search, beta, way, vol, res, image, mine, other, volume):
    total = norms[0, 0:1]
    for c in range(1, NC):
        total = total + norms[c, 0:1]
    alpha = per_frame(gamma[0:1] / total, VS)
    along = search[...] + per_frame(beta[0:1], VS) * way[...]
    volume[...] = vol[...] + alpha * along
    residual = res[...] - alpha[:, :RO] * image[...]
    mine[:, :VH] = volume[:, pl.ds(pl.multiple_of(k[0] * VH, VH), VH)]
    other[:, :VH] = volume[:, pl.ds(pl.multiple_of((1 - k[0]) * VH, VH), VH)]
    mine[:, VH:] = residual[:, :RS]
    other[:, VH:] = residual[:, RS:]


def finish_body(k, mine, other, volume, residual, turned):
    turned[pl.ds(pl.multiple_of(k[0] * FH, FH), FH)] = mine[...]
    turned[pl.ds(pl.multiple_of((1 - k[0]) * FH, FH), FH)] = other[...]
    whole = turned[...].T
    volume[...] = whole[:VH]
    residual[...] = whole[VH:]


def shifted(value, axis, by):
    n = lax.axis_size(axis)
    return lax.ppermute(value, axis, [(i, (i + by) % n) for i in range(n)])


def swapped(value, pairs):
    return lax.ppermute(value, "x", [(i, j) for a, b in pairs for i, j in ((a, b), (b, a))])


def exchanged(parts, axis):
    return lax.all_to_all(parts, axis, split_axis=0, concat_axis=0, tiled=True)


LINE = (8, LANES)
COLUMN = (NC, NK * FH + PAD, RS)
SHARD = (VROWS + PAD, LANES)


def local(tiles, tile_row, tile_col, tile_count, sinogram):
    x = lax.axis_index("x").astype(jnp.int32).reshape(1)
    k = lax.axis_index("k").astype(jnp.int32).reshape(1)
    line = shape(LINE, F32)
    rays = shape((FH, RO), F32)
    voxels = shape((FH, VS), F32)
    column = shape(COLUMN, BF)
    shard = shape(SHARD, BF)

    table = jnp.concatenate(
        [tile_row[0], tile_col[0], jnp.broadcast_to(tile_count, tile_row.shape[1:])], axis=0
    )
    half = shape((FH, RS), F32)
    mine, other = kernel(
        turn_body, "turn", (half, half), (k, sinogram[0]), (pltpu.VMEM((FRAMES, RS), F32),)
    )
    table2 = shifted(table, "k", 1)
    other = shifted(other, "k", 1)
    stored, other, table2, x = lax.optimization_barrier((tiles[0, 0], other, table2, x))
    stored2 = shifted(stored, "k", 1)
    residual, message = kernel(start_body, "start", (rays, column), (mine, other))
    arrived = exchanged(message, COL)
    dense, turned = build(x, table, table2, stored, stored2, arrived)

    def backward(arrived):
        field, norm, p2 = kernel(
            gather_body, "gather", (shape((FH, NK * RAYS), BF), line, shard), (arrived, dense), limit=8
        )

        def piece(j, out):
            return kernel(
                functools.partial(piece_body, j), f"piece{j}", out, (field, norm, dense), limit=8
            )

        far = shifted(p2, "x", 2)
        near = shifted(piece(1, shard), "x", 1)
        back = shifted(piece(3, shard), "x", 3)
        return piece(0, voxels), norm, near, back, far

    def forward(message):
        far = shifted(message, "x", 2)
        near = shifted(message, "x", 1)
        back = shifted(message, "x", 3)
        whole = shape((FH, NK * RAYS), F32)
        image = kernel(here_body, "here", whole, (message, turned), limit=8)
        image = kernel(beside_body, "beside", whole, (near, back, turned, image), limit=8)
        out = kernel(
            forward_body, "forward", column, (far, turned, image, message, near, back), limit=8
        )
        return exchanged(out, COL)

    search, shard_out, last = kernel(first_body, "first", (voxels, shard, line), backward(arrived))
    image, gamma, guess, message = kernel(
        image_first_body,
        "image_first",
        (rays, line, line, column),
        (forward(shard_out), residual, last),
    )
    beta = direction = volume = None
    for step in range(1, ITERS):
        state = (search, residual, image, gamma, guess)
        if step > 1:
            state += (beta, direction, volume)

        def body(*refs, first=step == 1):
            next_body(first, *refs)

        search, direction, volume, residual, shard_out, guess = kernel(
            body,
            "next",
            (voxels, voxels, voxels, rays, shard, line),
            (*backward(exchanged(message, COL)), *state),
        )
        arrived = forward(shard_out)
        if step + 1 < ITERS:
            image, gamma, beta, message = kernel(
                image_next_body,
                "image_next",
                (rays, line, line, column),
                (arrived, residual, guess, image, gamma),
            )
    image, gamma, beta, norm = kernel(
        image_last_body,
        "image_last",
        (rays, line, line, line),
        (arrived, image, gamma),
    )
    norm = kernel(pair_body, "pair", line, (norm, swapped(norm, ((0, 1), (2, 3)))))
    norms = kernel(
        pairs_body, "pairs", shape((NC, *LINE), F32), (norm, swapped(norm, ((1, 2), (3, 0))))
    )
    both = shape((FH, VH + RS), F32)
    mine, other = kernel(
        final_body,
        "final",
        (both, both),
        (k, exchanged(norms, COL), gamma, search, beta, direction, volume, residual, image),
        (pltpu.VMEM((FH, VS), F32),),
    )
    volume, residual = kernel(
        finish_body,
        "finish",
        (shape((VH, FRAMES), F32), shape((RS, FRAMES), F32)),
        (k, mine, shifted(other, "k", 1)),
        (pltpu.VMEM((FRAMES, VH + RS), F32),),
    )
    return volume[None], residual[None]


def solution(mesh):
    finer = Mesh(mesh.devices.reshape(4, 2, 4, 4), ("x", "k", "y", "z"))
    placed = (
        P(ROW, COL, None, None, None),
        P(ROW, COL, None),
        P(ROW, COL, None),
        P(ROW, COL),
        P(ROW, COL, None),
    )
    return jax.shard_map(
        local,
        mesh=finer,
        in_specs=placed,
        out_specs=(P(COL, ROW, None), P(ROW, COL, None)),
        check_vma=False,
    )
```

```python
import functools

import jax
import jax.numpy as jnp
from jax import lax
from jax.experimental import pallas as pl
from jax.experimental.pallas import tpu as pltpu
from jax.sharding import Mesh
from jax.sharding import PartitionSpec as P


ROW = ("x", "k")
COL = ("y", "z")
NX, NK, NC = 4, 2, 16
TILE = 128
RAYS = 2048
VOX = 2048
FRAMES = 128
ITERS = 4
FH = FRAMES // NK
RS = RAYS // NC
RO = NK * RS
VS = VOX // NX
VH = VS // NK
VROWS = VS // 128 * FH
PAD = 8
LANES = 128
BF = jnp.bfloat16
F32 = jnp.float32


def vmem():
    return pl.BlockSpec(memory_space=pltpu.VMEM)


def smem():
    return pl.BlockSpec(memory_space=pltpu.SMEM)


def hbm():
    return pl.BlockSpec(memory_space=pltpu.HBM)


def shape(dims, dtype):
    return jax.ShapeDtypeStruct(dims, dtype)


def kernel(body, outs, ins, scratch=(), limit=4):
    return pl.pallas_call(
        body,
        out_shape=outs,
        in_specs=[smem() if a.dtype == jnp.int32 else vmem() for a in ins],
        out_specs=jax.tree.map(lambda _: vmem(), outs),
        scratch_shapes=list(scratch),
        compiler_params=pltpu.CompilerParams(vmem_limit_bytes=limit << 20),
    )(*ins)


def squares(values):
    total = values[:, :LANES] * values[:, :LANES]
    for i in range(LANES, values.shape[1], LANES):
        total += values[:, i : i + LANES] * values[:, i : i + LANES]
    square = jnp.concatenate([total, jnp.zeros((LANES - FH, LANES), F32)], axis=0)
    return jnp.sum(square.T, axis=0, keepdims=True)


def per_frame(row, width):
    column = jnp.broadcast_to(row, (LANES, LANES)).T[:FH]
    return jnp.concatenate([column] * (width // LANES), axis=1)


def as_rows(row):
    high = row.astype(BF).astype(F32)
    rest = row - high
    mid = rest.astype(BF).astype(F32)
    low = rest - mid
    i = lax.broadcasted_iota(jnp.int32, (PAD, LANES), 0)
    zero = jnp.zeros((PAD, LANES), F32)
    return jnp.where(i == 0, high, jnp.where(i == 1, mid, jnp.where(i == 2, low, zero))).astype(BF)


def row_of(rows):
    return jnp.sum(rows.astype(F32), axis=0, keepdims=True)


def wide(row):
    return jnp.broadcast_to(row, (8, LANES))


def stacked(values):
    return jnp.concatenate(
        [values[:, i : i + LANES] for i in range(0, values.shape[1], LANES)], axis=0
    )


def unstacked(rows):
    return jnp.concatenate([rows[i : i + FH] for i in range(0, rows.shape[0], FH)], axis=1)


def put(message, values, row):
    message[: message.shape[0] - PAD] = stacked(values.astype(BF))
    message[message.shape[0] - PAD :] = as_rows(row)


def put_all(message, values, row):
    part = stacked(values.astype(BF))
    rows = as_rows(row)
    for c in range(NC):
        message[c, : RO // LANES * FH] = part
        message[c, RO // LANES * FH :] = rows


def turn_body(k, sino, mine, other, turned):
    turned[...] = sino[...].T
    mine[...] = turned[pl.ds(pl.multiple_of(k[0] * FH, FH), FH)]
    other[...] = turned[pl.ds(pl.multiple_of((1 - k[0]) * FH, FH), FH)]


def start_body(mine, other, residual, message):
    values = jnp.concatenate([mine[...], other[...]], axis=1)
    residual[...] = values
    put_all(message, values, squares(values))


def build_body(x, table, table2, tiles, tiles2, after, dense, sem, sem2):
    shift = x[0] * (NC // NX)
    halves = ((table, tiles, sem), (table2, tiles2, sem2))

    def copy(half, t):
        index, stored, done = halves[half]
        r = pl.multiple_of(index[0, t] * TILE + half * RAYS, TILE)
        c = pl.multiple_of((index[1, t] + NC - shift) % NC * TILE, TILE)
        return pltpu.make_async_copy(stored.at[t], dense.at[pl.ds(r, TILE), pl.ds(c, TILE)], done)

    for half in range(NK):

        def start(t, carry, half=half):
            copy(half, t).start()
            return carry

        dense[half * RAYS : (half + 1) * RAYS] = jnp.zeros((RAYS, VOX), BF)
        lax.fori_loop(0, halves[half][0][2, 0], start, 0)
    for half in range(NK):

        def wait(t, carry, half=half):
            copy(half, t).wait()
            return carry

        lax.fori_loop(0, halves[half][0][2, 0], wait, 0)


def build(x, table, table2, tiles, tiles2, after):
    return pl.pallas_call(
        build_body,
        name="build",
        out_shape=pltpu.VMEM((NK * RAYS, VOX), BF),
        in_specs=[smem(), smem(), smem(), hbm(), hbm(), vmem()],
        out_specs=vmem(),
        scratch_shapes=[pltpu.SemaphoreType.DMA(()), pltpu.SemaphoreType.DMA(())],
        compiler_params=pltpu.CompilerParams(vmem_limit_bytes=44 << 20),
    )(x, table, table2, tiles, tiles2, after)


def turned_body(half, dense, turned):
    def turn(j, carry):
        voxels = pl.ds(pl.multiple_of(j * TILE, TILE), TILE)
        here = pl.ds(pl.multiple_of(j * TILE + half * VOX // 2, TILE), TILE)
        for i in range(0, NK * RAYS, TILE):
            turned[voxels, i : i + TILE] = dense[i : i + TILE, here].T
        return carry

    lax.fori_loop(0, VOX // 2 // TILE, turn, 0)


def turned_half(half, dense):
    return pl.pallas_call(
        functools.partial(turned_body, half),
        out_shape=pltpu.VMEM((VOX // 2, NK * RAYS), BF),
        in_specs=[vmem()],
        out_specs=vmem(),
        compiler_params=pltpu.CompilerParams(vmem_limit_bytes=4 << 20),
    )(dense)


def gather_body(arrived, dense, field, norm, far):
    seen = arrived[0, NK * FH :].astype(F32)
    for c in range(NC):
        for h in range(NK):
            field[:, h * RAYS + c * RS : h * RAYS + (c + 1) * RS] = arrived[c, h * FH : (h + 1) * FH]
        if c:
            seen += arrived[c, NK * FH :].astype(F32)
    row = row_of(seen)
    norm[...] = wide(row)
    part = jnp.dot(field[...], dense[:, 2 * VS : 3 * VS], preferred_element_type=F32)
    put(far, part, row)


def piece_body(j, field, norm, dense, out):
    part = jnp.dot(field[...], dense[:, j * VS : (j + 1) * VS], preferred_element_type=F32)
    if j:
        put(out, part, norm[0:1])
    else:
        out[...] = part


def arrived_sum(own, norm, pieces):
    value = own[...]
    row = norm[0:1]
    for p in pieces:
        value = value + unstacked(p[:VROWS].astype(F32))
        row = row + row_of(p[VROWS:])
    return value, row


def first_body(own, norm, p1, p2, p3, search, message, total):
    value, row = arrived_sum(own, norm, (p1, p2, p3))
    search[...] = value
    put(message, value, squares(value))
    total[...] = wide(row)


def next_body(first, own, norm, p1, p2, p3, *refs):
    if first:
        old, res, image, gamma, guess = refs[:5]
        outs = refs[5:]
    else:
        old, res, image, gamma, guess, beta, way, vol = refs[:8]
        outs = refs[8:]
    search, direction, volume, residual, message, step = outs
    value, row = arrived_sum(own, norm, (p1, p2, p3))
    alpha = gamma[0:1] / row
    ratio = per_frame(alpha / guess[0:1], VS)
    fresh = (1.0 - ratio) * old[...] + ratio * value
    search[...] = fresh
    put(message, fresh, squares(fresh))
    scale = per_frame(alpha, VS)
    if first:
        along = old[...]
        volume[...] = scale * along
    else:
        along = old[...] + per_frame(beta[0:1], VS) * way[...]
        volume[...] = vol[...] + scale * along
    direction[...] = along
    residual[...] = res[...] - scale[:, :RO] * image[...]
    step[...] = wide(alpha)


SIZE = 4 * RS


def part_of(places, messages, turned, at):
    total = None
    for j, m in zip(places, messages):
        part = jnp.dot(
            unstacked(m[:VROWS]),
            turned[j // 2][j % 2 * VS : (j % 2 + 1) * VS, at : at + SIZE],
            preferred_element_type=F32,
        )
        total = part if total is None else total + part
    return total


def here_body(here, turned0, image):
    for at in range(0, NK * RAYS, SIZE):
        image[:, at : at + SIZE] = part_of((0,), (here,), (turned0, None), at)


def far_body(far, turned1, so_far, image):
    for at in range(0, NK * RAYS, SIZE):
        part = part_of((2,), (far,), (None, turned1), at)
        image[:, at : at + SIZE] = so_far[:, at : at + SIZE] + part


def forward_body(near, back, turned0, turned1, so_far, here, far, out):
    row = jnp.zeros((1, LANES), F32)
    for m in (here, near, back, far):
        row = row + row_of(m[VROWS:])
    rows = as_rows(row)
    for c in range(NC):
        out[c, NK * FH :] = rows
    for at in range(0, NK * RAYS, SIZE):
        part = part_of((3, 1), (near, back), (turned0, turned1), at)
        part = (part + so_far[:, at : at + SIZE]).astype(BF)
        h, first = at // RAYS, at % RAYS // RS
        for c in range(SIZE // RS):
            out[first + c, h * FH : (h + 1) * FH] = part[:, c * RS : (c + 1) * RS]


def gathered(arrived):
    value = arrived[0].astype(F32)
    for c in range(1, NC):
        value = value + arrived[c].astype(F32)
    return unstacked(value[: NK * FH]), jnp.sum(value[NK * FH :], axis=0, keepdims=True)


def image_first_body(arrived, res, last, image, gamma, guess, message):
    value, row = gathered(arrived)
    image[...] = value
    gamma[...] = wide(row)
    about = last[0:1] / row
    about = jnp.where((about > 0.0) & (about < jnp.inf), about, 1.0)
    guess[...] = wide(about)
    put_all(message, res[...] - per_frame(about, RO) * value, squares(value))


def image_next_body(arrived, res, about, previous, last, image, gamma, beta, message):
    value, row = gathered(arrived)
    ratio = row / last[0:1]
    value = value + per_frame(ratio, RO) * previous[...]
    image[...] = value
    gamma[...] = wide(row)
    beta[...] = wide(ratio)
    put_all(message, res[...] - per_frame(about[0:1], RO) * value, squares(value))


def image_last_body(arrived, previous, last, image, gamma, beta, norms):
    value, row = gathered(arrived)
    ratio = row / last[0:1]
    value = value + per_frame(ratio, RO) * previous[...]
    image[...] = value
    gamma[...] = wide(row)
    beta[...] = wide(ratio)
    norm = wide(squares(value))
    for x in range(NX):
        norms[x] = norm


def norm_body(arrived, norms):
    total = arrived[0]
    for x in range(1, NX):
        total = total + arrived[x]
    for c in range(NC):
        norms[c] = total


def final_body(k, norms, gamma, search, beta, way, vol, res, image, mine, other, volume):
    total = norms[0, 0:1]
    for c in range(1, NC):
        total = total + norms[c, 0:1]
    alpha = per_frame(gamma[0:1] / total, VS)
    along = search[...] + per_frame(beta[0:1], VS) * way[...]
    volume[...] = vol[...] + alpha * along
    residual = res[...] - alpha[:, :RO] * image[...]
    mine[:, :VH] = volume[:, pl.ds(pl.multiple_of(k[0] * VH, VH), VH)]
    other[:, :VH] = volume[:, pl.ds(pl.multiple_of((1 - k[0]) * VH, VH), VH)]
    mine[:, VH:] = residual[:, :RS]
    other[:, VH:] = residual[:, RS:]


def finish_body(k, mine, other, volume, residual, turned):
    turned[pl.ds(pl.multiple_of(k[0] * FH, FH), FH)] = mine[...]
    turned[pl.ds(pl.multiple_of((1 - k[0]) * FH, FH), FH)] = other[...]
    whole = turned[...].T
    volume[...] = whole[:VH]
    residual[...] = whole[VH:]


def shifted(value, axis, by):
    n = lax.axis_size(axis)
    return lax.ppermute(value, axis, [(i, (i + by) % n) for i in range(n)])


def exchanged(parts, axis):
    return lax.all_to_all(parts, axis, split_axis=0, concat_axis=0, tiled=True)


LINE = (8, LANES)
COLUMN = (NC, NK * FH + PAD, RS)
SHARD = (VROWS + PAD, LANES)


def local(tiles, tile_row, tile_col, tile_count, sinogram):
    x = lax.axis_index("x").astype(jnp.int32).reshape(1)
    k = lax.axis_index("k").astype(jnp.int32).reshape(1)
    line = shape(LINE, F32)
    rays = shape((FH, RO), F32)
    voxels = shape((FH, VS), F32)
    column = shape(COLUMN, BF)
    shard = shape(SHARD, BF)

    table = jnp.concatenate(
        [tile_row[0], tile_col[0], jnp.broadcast_to(tile_count, tile_row.shape[1:])], axis=0
    )
    half = shape((FH, RS), F32)
    mine, other = kernel(
        turn_body, (half, half), (k, sinogram[0]), (pltpu.VMEM((FRAMES, RS), F32),)
    )
    table2 = shifted(table, "k", 1)
    other = shifted(other, "k", 1)
    stored, other, table2, x = lax.optimization_barrier((tiles[0, 0], other, table2, x))
    stored2 = shifted(stored, "k", 1)
    residual, message = kernel(start_body, (rays, column), (mine, other))
    arrived = exchanged(message, COL)
    dense = build(x, table, table2, stored, stored2, arrived)
    turned = (turned_half(0, dense), turned_half(1, dense))

    def backward_of(arrived):
        field, norm, p2 = kernel(
            gather_body, (shape((FH, NK * RAYS), BF), line, shard), (arrived, dense), limit=8
        )

        def piece(j, out):
            return kernel(functools.partial(piece_body, j), out, (field, norm, dense), limit=8)

        far = shifted(p2, "x", 2)
        p1 = piece(1, shard)
        near = shifted(p1, "x", 1)
        p3 = piece(3, shard)
        back = shifted(p3, "x", 3)
        return piece(0, voxels), norm, far, near, back

    def forward(message):
        far = shifted(message, "x", 2)
        near = shifted(message, "x", 1)
        back = shifted(message, "x", 3)
        whole = shape((FH, NK * RAYS), F32)
        image = kernel(here_body, whole, (message, turned[0]), limit=8)
        image = kernel(far_body, whole, (far, turned[1], image), limit=8)
        out = kernel(forward_body, column, (near, back, *turned, image, message, far), limit=8)
        return exchanged(out, COL)

    search, shard_out, last = kernel(first_body, (voxels, shard, line), backward_of(arrived))
    image, gamma, guess, message = kernel(
        image_first_body, (rays, line, line, column), (forward(shard_out), residual, last)
    )
    beta = direction = volume = None
    for step in range(1, ITERS):
        state = (search, residual, image, gamma, guess)
        if step > 1:
            state += (beta, direction, volume)

        def body(*refs, first=step == 1):
            next_body(first, *refs)

        search, direction, volume, residual, shard_out, guess = kernel(
            body,
            (voxels, voxels, voxels, rays, shard, line),
            (*backward_of(exchanged(message, COL)), *state),
        )
        arrived = forward(shard_out)
        if step + 1 < ITERS:
            image, gamma, beta, message = kernel(
                image_next_body,
                (rays, line, line, column),
                (arrived, residual, guess, image, gamma),
            )
    image, gamma, beta, norms = kernel(
        image_last_body, (rays, line, line, shape((NX, *LINE), F32)), (arrived, image, gamma)
    )
    norms = kernel(norm_body, shape((NC, *LINE), F32), (exchanged(norms, "x"),))
    both = shape((FH, VH + RS), F32)
    mine, other = kernel(
        final_body,
        (both, both),
        (k, exchanged(norms, COL), gamma, search, beta, direction, volume, residual, image),
        (pltpu.VMEM((FH, VS), F32),),
    )
    volume, residual = kernel(
        finish_body,
        (shape((VH, FRAMES), F32), shape((RS, FRAMES), F32)),
        (k, mine, shifted(other, "k", 1)),
        (pltpu.VMEM((FRAMES, VH + RS), F32),),
    )
    return volume[None], residual[None]


def solution(mesh):
    finer = Mesh(mesh.devices.reshape(4, 2, 4, 4), ("x", "k", "y", "z"))
    placed = (
        P(ROW, COL, None, None, None),
        P(ROW, COL, None),
        P(ROW, COL, None),
        P(ROW, COL),
        P(ROW, COL, None),
    )
    return jax.shard_map(
        local,
        mesh=finer,
        in_specs=placed,
        out_specs=(P(COL, ROW, None), P(ROW, COL, None)),
        check_vma=False,
    )
```

```python
import functools

import jax
import jax.numpy as jnp
from jax import lax
from jax.experimental import pallas as pl
from jax.experimental.pallas import tpu as pltpu
from jax.sharding import Mesh
from jax.sharding import PartitionSpec as P


ROW = ("x", "k")
COL = ("y", "z")
NX, NK, NC = 4, 2, 16
TILE = 128
RAYS = 2048
VOX = 2048
FRAMES = 128
ITERS = 4
FH = FRAMES // NK
RS = RAYS // NC
RO = NK * RS
VS = VOX // NX
VH = VS // NK
VROWS = VS // 128 * FH
PAD = 8
LANES = 128
BF = jnp.bfloat16
F32 = jnp.float32


def vmem():
    return pl.BlockSpec(memory_space=pltpu.VMEM)


def smem():
    return pl.BlockSpec(memory_space=pltpu.SMEM)


def hbm():
    return pl.BlockSpec(memory_space=pltpu.HBM)


def shape(dims, dtype):
    return jax.ShapeDtypeStruct(dims, dtype)


def kernel(body, outs, ins, scratch=(), limit=4):
    return pl.pallas_call(
        body,
        out_shape=outs,
        in_specs=[smem() if a.dtype == jnp.int32 else vmem() for a in ins],
        out_specs=jax.tree.map(lambda _: vmem(), outs),
        scratch_shapes=list(scratch),
        compiler_params=pltpu.CompilerParams(vmem_limit_bytes=limit << 20),
    )(*ins)


def squares(values):
    total = values[:, :LANES] * values[:, :LANES]
    for i in range(LANES, values.shape[1], LANES):
        total += values[:, i : i + LANES] * values[:, i : i + LANES]
    square = jnp.concatenate([total, jnp.zeros((LANES - FH, LANES), F32)], axis=0)
    return jnp.sum(square.T, axis=0, keepdims=True)


def per_frame(row, width):
    column = jnp.broadcast_to(row, (LANES, LANES)).T[:FH]
    return jnp.concatenate([column] * (width // LANES), axis=1)


def as_rows(row):
    high = row.astype(BF).astype(F32)
    rest = row - high
    mid = rest.astype(BF).astype(F32)
    low = rest - mid
    i = lax.broadcasted_iota(jnp.int32, (PAD, LANES), 0)
    zero = jnp.zeros((PAD, LANES), F32)
    return jnp.where(i == 0, high, jnp.where(i == 1, mid, jnp.where(i == 2, low, zero))).astype(BF)


def row_of(rows):
    return jnp.sum(rows.astype(F32), axis=0, keepdims=True)


def wide(row):
    return jnp.broadcast_to(row, (8, LANES))


def stacked(values):
    return jnp.concatenate(
        [values[:, i : i + LANES] for i in range(0, values.shape[1], LANES)], axis=0
    )


def unstacked(rows):
    return jnp.concatenate([rows[i : i + FH] for i in range(0, rows.shape[0], FH)], axis=1)


def put(message, values, row):
    message[: message.shape[0] - PAD] = stacked(values.astype(BF))
    message[message.shape[0] - PAD :] = as_rows(row)


def put_all(message, values, row):
    part = stacked(values.astype(BF))
    rows = as_rows(row)
    for c in range(NC):
        message[c, : RO // LANES * FH] = part
        message[c, RO // LANES * FH :] = rows


def turn_body(k, count, rows, cols, sino, mine, other, table, turned, rows_in, cols_in, sino_in, sems):
    copies = [
        pltpu.make_async_copy(source, target, sems.at[i])
        for i, (source, target) in enumerate(((sino, sino_in), (rows, rows_in), (cols, cols_in)))
    ]
    for copy in copies:
        copy.start()
    for copy in copies:
        copy.wait()
    turned[...] = sino_in[...].T
    mine[...] = turned[pl.ds(pl.multiple_of(k[0] * FH, FH), FH)]
    other[:FH] = turned[pl.ds(pl.multiple_of((1 - k[0]) * FH, FH), FH)]
    i = lax.broadcasted_iota(jnp.int32, (8, LANES), 0)
    stored = jnp.where(i == 0, rows_in[...], jnp.where(i == 1, cols_in[...], count[0, 0]))
    table[...] = stored
    other[FH:] = stored.astype(F32)


def start_body(mine, other, residual, message, table):
    values = jnp.concatenate([mine[...], other[:FH]], axis=1)
    residual[...] = values
    put_all(message, values, squares(values))
    table[...] = other[FH:].astype(jnp.int32)


def build_body(x, table, table2, tiles, tiles2, after, dense, sem, sem2):
    shift = x[0] * (NC // NX)
    halves = ((table, tiles, sem), (table2, tiles2, sem2))

    def copy(half, t):
        index, stored, done = halves[half]
        r = pl.multiple_of(index[0, t] * TILE + half * RAYS, TILE)
        c = pl.multiple_of((index[1, t] + NC - shift) % NC * TILE, TILE)
        return pltpu.make_async_copy(stored.at[t], dense.at[pl.ds(r, TILE), pl.ds(c, TILE)], done)

    for half in range(NK):

        def start(t, carry, half=half):
            copy(half, t).start()
            return carry

        dense[half * RAYS : (half + 1) * RAYS] = jnp.zeros((RAYS, VOX), BF)
        lax.fori_loop(0, halves[half][0][2, 0], start, 0)
    for half in range(NK):

        def wait(t, carry, half=half):
            copy(half, t).wait()
            return carry

        lax.fori_loop(0, halves[half][0][2, 0], wait, 0)


def build(x, table, table2, tiles, tiles2, after):
    return pl.pallas_call(
        build_body,
        name="build",
        out_shape=pltpu.VMEM((NK * RAYS, VOX), BF),
        in_specs=[smem(), smem(), smem(), hbm(), hbm(), vmem()],
        out_specs=vmem(),
        scratch_shapes=[pltpu.SemaphoreType.DMA(()), pltpu.SemaphoreType.DMA(())],
        compiler_params=pltpu.CompilerParams(vmem_limit_bytes=44 << 20),
    )(x, table, table2, tiles, tiles2, after)


def turned_body(half, dense, turned):
    def turn(j, carry):
        voxels = pl.ds(pl.multiple_of(j * TILE, TILE), TILE)
        here = pl.ds(pl.multiple_of(j * TILE + half * VOX // 2, TILE), TILE)
        for i in range(0, NK * RAYS, TILE):
            turned[voxels, i : i + TILE] = dense[i : i + TILE, here].T
        return carry

    lax.fori_loop(0, VOX // 2 // TILE, turn, 0)


def turned_half(half, dense):
    return pl.pallas_call(
        functools.partial(turned_body, half),
        out_shape=pltpu.VMEM((VOX // 2, NK * RAYS), BF),
        in_specs=[vmem()],
        out_specs=vmem(),
        compiler_params=pltpu.CompilerParams(vmem_limit_bytes=4 << 20),
    )(dense)


def gather_body(arrived, dense, field, norm, far):
    seen = arrived[0, NK * FH :].astype(F32)
    for c in range(NC):
        for h in range(NK):
            field[:, h * RAYS + c * RS : h * RAYS + (c + 1) * RS] = arrived[c, h * FH : (h + 1) * FH]
        if c:
            seen += arrived[c, NK * FH :].astype(F32)
    row = row_of(seen)
    norm[...] = wide(row)
    part = jnp.dot(field[...], dense[:, 2 * VS : 3 * VS], preferred_element_type=F32)
    put(far, part, row)


def piece_body(j, field, norm, dense, out):
    part = jnp.dot(field[...], dense[:, j * VS : (j + 1) * VS], preferred_element_type=F32)
    if j:
        put(out, part, norm[0:1])
    else:
        out[...] = part


def arrived_sum(own, norm, pieces):
    value = own[...]
    row = norm[0:1]
    for p in pieces:
        value = value + unstacked(p[:VROWS].astype(F32))
        row = row + row_of(p[VROWS:])
    return value, row


def first_body(own, norm, p1, p2, p3, search, message, total):
    value, row = arrived_sum(own, norm, (p1, p2, p3))
    search[...] = value
    put(message, value, squares(value))
    total[...] = wide(row)


def next_body(own, norm, p1, p2, p3, old, gamma, guess, search, message, step):
    value, row = arrived_sum(own, norm, (p1, p2, p3))
    alpha = gamma[0:1] / row
    ratio = per_frame(alpha / guess[0:1], VS)
    fresh = (1.0 - ratio) * old[...] + ratio * value
    search[...] = fresh
    put(message, fresh, squares(fresh))
    step[...] = wide(alpha)


def update_body(first, step, old, res, image, *refs):
    direction, volume, residual = refs[-3:]
    alpha = per_frame(step[0:1], VS)
    if first:
        along = old[...]
        volume[...] = alpha * along
    else:
        beta, way, vol = refs[:3]
        along = old[...] + per_frame(beta[0:1], VS) * way[...]
        volume[...] = vol[...] + alpha * along
    direction[...] = along
    residual[...] = res[...] - alpha[:, :RO] * image[...]


SIZE = 4 * RS


def part_of(j, message, turned, at):
    first = j % 2 * VS
    return jnp.dot(
        unstacked(message[:VROWS]),
        turned[first : first + VS, at : at + SIZE],
        preferred_element_type=F32,
    )


def product_body(j, message, turned, *refs):
    image = refs[-1]
    for at in range(0, NK * RAYS, SIZE):
        part = part_of(j, message, turned, at)
        if len(refs) > 1:
            part = part + refs[0][:, at : at + SIZE]
        image[:, at : at + SIZE] = part


def forward_body(j, message, turned, so_far, m1, m2, m3, out):
    row = jnp.zeros((1, LANES), F32)
    for m in (message, m1, m2, m3):
        row = row + row_of(m[VROWS:])
    rows = as_rows(row)
    for c in range(NC):
        out[c, NK * FH :] = rows
    for at in range(0, NK * RAYS, SIZE):
        part = (part_of(j, message, turned, at) + so_far[:, at : at + SIZE]).astype(BF)
        h, first = at // RAYS, at % RAYS // RS
        for c in range(SIZE // RS):
            out[first + c, h * FH : (h + 1) * FH] = part[:, c * RS : (c + 1) * RS]


def gathered(arrived):
    value = arrived[0].astype(F32)
    for c in range(1, NC):
        value = value + arrived[c].astype(F32)
    return unstacked(value[: NK * FH]), jnp.sum(value[NK * FH :], axis=0, keepdims=True)


def image_first_body(arrived, res, last, image, gamma, guess, message):
    value, row = gathered(arrived)
    image[...] = value
    gamma[...] = wide(row)
    about = last[0:1] / row
    about = jnp.where((about > 0.0) & (about < jnp.inf), about, 1.0)
    guess[...] = wide(about)
    put_all(message, res[...] - per_frame(about, RO) * value, squares(value))


def image_next_body(arrived, res, about, previous, last, image, gamma, beta, message):
    value, row = gathered(arrived)
    ratio = row / last[0:1]
    value = value + per_frame(ratio, RO) * previous[...]
    image[...] = value
    gamma[...] = wide(row)
    beta[...] = wide(ratio)
    put_all(message, res[...] - per_frame(about[0:1], RO) * value, squares(value))


def image_last_body(arrived, previous, last, image, gamma, beta, norm):
    value, row = gathered(arrived)
    ratio = row / last[0:1]
    value = value + per_frame(ratio, RO) * previous[...]
    image[...] = value
    gamma[...] = wide(row)
    beta[...] = wide(ratio)
    norm[...] = wide(squares(value))


def norm_body(mine, far, near, back, norms):
    total = mine[...] + far[...] + near[...] + back[...]
    for c in range(NC):
        norms[c] = total


def final_body(k, norms, gamma, search, beta, way, vol, res, image, mine, other, volume):
    total = norms[0, 0:1]
    for c in range(1, NC):
        total = total + norms[c, 0:1]
    alpha = per_frame(gamma[0:1] / total, VS)
    along = search[...] + per_frame(beta[0:1], VS) * way[...]
    volume[...] = vol[...] + alpha * along
    residual = res[...] - alpha[:, :RO] * image[...]
    mine[:, :VH] = volume[:, pl.ds(pl.multiple_of(k[0] * VH, VH), VH)]
    other[:, :VH] = volume[:, pl.ds(pl.multiple_of((1 - k[0]) * VH, VH), VH)]
    mine[:, VH:] = residual[:, :RS]
    other[:, VH:] = residual[:, RS:]


def finish_body(k, mine, other, volume, residual, turned):
    turned[pl.ds(pl.multiple_of(k[0] * FH, FH), FH)] = mine[...]
    turned[pl.ds(pl.multiple_of((1 - k[0]) * FH, FH), FH)] = other[...]
    whole = turned[...].T
    volume[...] = whole[:VH]
    residual[...] = whole[VH:]


def shifted(value, axis, by):
    n = lax.axis_size(axis)
    return lax.ppermute(value, axis, [(i, (i + by) % n) for i in range(n)])


def exchanged(parts, axis):
    return lax.all_to_all(parts, axis, split_axis=0, concat_axis=0, tiled=True)


LINE = (8, LANES)
COLUMN = (NC, NK * FH + PAD, RS)
SHARD = (VROWS + PAD, LANES)


def local(tiles, tile_row, tile_col, tile_count, sinogram):
    x = lax.axis_index("x").astype(jnp.int32).reshape(1)
    k = lax.axis_index("k").astype(jnp.int32).reshape(1)
    line = shape(LINE, F32)
    rays = shape((FH, RO), F32)
    voxels = shape((FH, VS), F32)
    column = shape(COLUMN, BF)
    shard = shape(SHARD, BF)

    table_shape = shape((8, LANES), jnp.int32)
    mine, other, table = pl.pallas_call(
        turn_body,
        name="turn",
        out_shape=(shape((FH, RS), F32), shape((FH + 8, RS), F32), table_shape),
        in_specs=[smem(), smem(), hbm(), hbm(), hbm()],
        out_specs=(vmem(), vmem(), vmem()),
        scratch_shapes=[
            pltpu.VMEM((FRAMES, RS), F32),
            pltpu.VMEM((1, LANES), jnp.int32),
            pltpu.VMEM((1, LANES), jnp.int32),
            pltpu.VMEM((RS, FRAMES), F32),
            pltpu.SemaphoreType.DMA((3,)),
        ],
        compiler_params=pltpu.CompilerParams(vmem_limit_bytes=61 << 20),
    )(k, tile_count, tile_row[0], tile_col[0], sinogram[0])
    other = shifted(other, "k", 1)
    stored, other, x = lax.optimization_barrier((tiles[0, 0], other, x))
    stored2 = shifted(stored, "k", 1)
    residual, message, table2 = kernel(
        start_body, (rays, column, table_shape), (mine, other), limit=61
    )
    arrived = exchanged(message, COL)
    dense = build(x, table, table2, stored, stored2, arrived)
    turned = (turned_half(0, dense), turned_half(1, dense))

    def backward_of(arrived):
        field, norm, p2 = kernel(
            gather_body, (shape((FH, NK * RAYS), BF), line, shard), (arrived, dense), limit=8
        )

        def piece(j, out):
            return kernel(functools.partial(piece_body, j), out, (field, norm, dense), limit=8)

        far = shifted(p2, "x", 2)
        p1 = piece(1, shard)
        near = shifted(p1, "x", 1)
        p3 = piece(3, shard)
        back = shifted(p3, "x", 3)
        return piece(0, voxels), norm, far, near, back

    def forward(message, update=None):
        return forward_of(message, update)

    def forward_of(message, update):
        far = shifted(message, "x", 2)
        near = shifted(message, "x", 1)
        back = shifted(message, "x", 3)
        whole = shape((FH, NK * RAYS), F32)

        def product(j, message, *so_far):
            return kernel(
                functools.partial(product_body, j),
                whole,
                (message, turned[j // 2], *so_far),
                limit=8,
            )

        image = product(0, message)
        updated = None
        if update is not None:
            updated = update()
        image = product(3, near, image)
        image = product(2, far, image)
        out = kernel(
            functools.partial(forward_body, 1),
            column,
            (back, turned[0], image, message, near, far),
            limit=8,
        )
        return exchanged(out, COL), updated

    search, shard_out, last = kernel(first_body, (voxels, shard, line), backward_of(arrived))
    image, gamma, guess, message = kernel(
        image_first_body, (rays, line, line, column), (forward(shard_out)[0], residual, last)
    )
    beta = direction = volume = None
    for step in range(1, ITERS):
        old = search
        search, shard_out, guess = kernel(
            next_body,
            (voxels, shard, line),
            (*backward_of(exchanged(message, COL)), old, gamma, guess),
        )
        state = (guess, old, residual, image)
        if step > 1:
            state += (beta, direction, volume)

        def update(state=state, first=step == 1):
            return kernel(functools.partial(update_body, first), (voxels, voxels, rays), state)

        arrived, (direction, volume, residual) = forward(shard_out, update)
        if step + 1 < ITERS:
            image, gamma, beta, message = kernel(
                image_next_body,
                (rays, line, line, column),
                (arrived, residual, guess, image, gamma),
            )
    image, gamma, beta, norm = kernel(
        image_last_body, (rays, line, line, line), (arrived, image, gamma)
    )
    others = tuple(shifted(norm, "x", j) for j in (2, 1, 3))
    norms = kernel(norm_body, shape((NC, *LINE), F32), (norm, *others))
    both = shape((FH, VH + RS), F32)
    mine, other = kernel(
        final_body,
        (both, both),
        (k, exchanged(norms, COL), gamma, search, beta, direction, volume, residual, image),
        (pltpu.VMEM((FH, VS), F32),),
    )
    volume, residual = kernel(
        finish_body,
        (shape((VH, FRAMES), F32), shape((RS, FRAMES), F32)),
        (k, mine, shifted(other, "k", 1)),
        (pltpu.VMEM((FRAMES, VH + RS), F32),),
    )
    return volume[None], residual[None]


def solution(mesh):
    finer = Mesh(mesh.devices.reshape(4, 2, 4, 4), ("x", "k", "y", "z"))
    placed = (
        P(ROW, COL, None, None, None),
        P(ROW, COL, None),
        P(ROW, COL, None),
        P(ROW, COL),
        P(ROW, COL, None),
    )
    return jax.shard_map(
        local,
        mesh=finer,
        in_specs=placed,
        out_specs=(P(COL, ROW, None), P(ROW, COL, None)),
        check_vma=False,
    )
```

```python
import functools

import jax
import jax.numpy as jnp
from jax import lax
from jax.experimental import pallas as pl
from jax.experimental.pallas import tpu as pltpu
from jax.sharding import Mesh
from jax.sharding import PartitionSpec as P


ROW = ("x", "k")
COL = ("y", "z")
NX, NK, NC = 4, 2, 16
TILE = 128
RAYS = 2048
VOX = 2048
FRAMES = 128
ITERS = 4
FH = FRAMES // NK
RS = RAYS // NC
RO = NK * RS
VS = VOX // NX
VH = VS // NK
VROWS = VS // 128 * FH
PAD = 8
LANES = 128
BF = jnp.bfloat16
F32 = jnp.float32


def vmem():
    return pl.BlockSpec(memory_space=pltpu.VMEM)


def smem():
    return pl.BlockSpec(memory_space=pltpu.SMEM)


def hbm():
    return pl.BlockSpec(memory_space=pltpu.HBM)


def shape(dims, dtype):
    return jax.ShapeDtypeStruct(dims, dtype)


def kernel(body, outs, ins, scratch=(), limit=4):
    return pl.pallas_call(
        body,
        out_shape=outs,
        in_specs=[smem() if a.dtype == jnp.int32 else vmem() for a in ins],
        out_specs=jax.tree.map(lambda _: vmem(), outs),
        scratch_shapes=list(scratch),
        compiler_params=pltpu.CompilerParams(vmem_limit_bytes=limit << 20),
    )(*ins)


def squares(values):
    total = values[:, :LANES] * values[:, :LANES]
    for i in range(LANES, values.shape[1], LANES):
        total += values[:, i : i + LANES] * values[:, i : i + LANES]
    square = jnp.concatenate([total, jnp.zeros((LANES - FH, LANES), F32)], axis=0)
    return jnp.sum(square.T, axis=0, keepdims=True)


def per_frame(row, width):
    column = jnp.broadcast_to(row, (LANES, LANES)).T[:FH]
    return jnp.concatenate([column] * (width // LANES), axis=1)


def as_rows(row):
    high = row.astype(BF).astype(F32)
    rest = row - high
    mid = rest.astype(BF).astype(F32)
    low = rest - mid
    i = lax.broadcasted_iota(jnp.int32, (PAD, LANES), 0)
    zero = jnp.zeros((PAD, LANES), F32)
    return jnp.where(i == 0, high, jnp.where(i == 1, mid, jnp.where(i == 2, low, zero))).astype(BF)


def row_of(rows):
    return jnp.sum(rows.astype(F32), axis=0, keepdims=True)


def wide(row):
    return jnp.broadcast_to(row, (8, LANES))


def stacked(values):
    return jnp.concatenate(
        [values[:, i : i + LANES] for i in range(0, values.shape[1], LANES)], axis=0
    )


def unstacked(rows):
    return jnp.concatenate([rows[i : i + FH] for i in range(0, rows.shape[0], FH)], axis=1)


def put(message, values, row):
    message[: message.shape[0] - PAD] = stacked(values.astype(BF))
    message[message.shape[0] - PAD :] = as_rows(row)


def put_all(message, values, row):
    part = stacked(values.astype(BF))
    rows = as_rows(row)
    for c in range(NC):
        message[c, : RO // LANES * FH] = part
        message[c, RO // LANES * FH :] = rows


def turn_body(k, sino, mine, other, turned):
    turned[...] = sino[...].T
    mine[...] = turned[pl.ds(pl.multiple_of(k[0] * FH, FH), FH)]
    other[...] = turned[pl.ds(pl.multiple_of((1 - k[0]) * FH, FH), FH)]


def start_body(mine, other, residual, message):
    values = jnp.concatenate([mine[...], other[...]], axis=1)
    residual[...] = values
    put_all(message, values, squares(values))


def build_body(x, table, table2, tiles, tiles2, after, dense, sem, sem2):
    halves = ((table, tiles, sem), (table2, tiles2, sem2))

    def copy(half, t):
        index, stored, done = halves[half]
        r = pl.multiple_of(index[0, t] * TILE + half * RAYS, TILE)
        piece = index[1, t] // (VS // TILE) ^ x[0]
        c = pl.multiple_of(piece * VS + index[1, t] % (VS // TILE) * TILE, TILE)
        return pltpu.make_async_copy(stored.at[t], dense.at[pl.ds(r, TILE), pl.ds(c, TILE)], done)

    for half in range(NK):

        def start(t, carry, half=half):
            copy(half, t).start()
            return carry

        dense[half * RAYS : (half + 1) * RAYS] = jnp.zeros((RAYS, VOX), BF)
        lax.fori_loop(0, halves[half][0][2, 0], start, 0)
    for half in range(NK):

        def wait(t, carry, half=half):
            copy(half, t).wait()
            return carry

        lax.fori_loop(0, halves[half][0][2, 0], wait, 0)


def build(x, table, table2, tiles, tiles2, after):
    return pl.pallas_call(
        build_body,
        name="build",
        out_shape=pltpu.VMEM((NK * RAYS, VOX), BF),
        in_specs=[smem(), smem(), smem(), hbm(), hbm(), vmem()],
        out_specs=vmem(),
        scratch_shapes=[pltpu.SemaphoreType.DMA(()), pltpu.SemaphoreType.DMA(())],
        compiler_params=pltpu.CompilerParams(vmem_limit_bytes=44 << 20),
    )(x, table, table2, tiles, tiles2, after)


def turned_body(half, dense, turned):
    def turn(j, carry):
        voxels = pl.ds(pl.multiple_of(j * TILE, TILE), TILE)
        here = pl.ds(pl.multiple_of(j * TILE + half * VOX // 2, TILE), TILE)
        for i in range(0, NK * RAYS, TILE):
            turned[voxels, i : i + TILE] = dense[i : i + TILE, here].T
        return carry

    lax.fori_loop(0, VOX // 2 // TILE, turn, 0)


def turned_half(half, dense):
    return pl.pallas_call(
        functools.partial(turned_body, half),
        out_shape=pltpu.VMEM((VOX // 2, NK * RAYS), BF),
        in_specs=[vmem()],
        out_specs=vmem(),
        compiler_params=pltpu.CompilerParams(vmem_limit_bytes=4 << 20),
    )(dense)


def gather_body(arrived, dense, field, norm, far):
    seen = arrived[0, NK * FH :].astype(F32)
    for c in range(NC):
        for h in range(NK):
            field[:, h * RAYS + c * RS : h * RAYS + (c + 1) * RS] = arrived[c, h * FH : (h + 1) * FH]
        if c:
            seen += arrived[c, NK * FH :].astype(F32)
    row = row_of(seen)
    norm[...] = wide(row)
    part = jnp.dot(field[...], dense[:, 2 * VS : 3 * VS], preferred_element_type=F32)
    put(far, part, row)


def piece_body(j, field, norm, dense, out):
    part = jnp.dot(field[...], dense[:, j * VS : (j + 1) * VS], preferred_element_type=F32)
    if j:
        put(out, part, norm[0:1])
    else:
        out[...] = part


def arrived_sum(own, norm, pieces):
    value = own[...]
    row = norm[0:1]
    for p in pieces:
        value = value + unstacked(p[:VROWS].astype(F32))
        row = row + row_of(p[VROWS:])
    return value, row


def first_body(own, norm, p1, p2, p3, search, message, total):
    value, row = arrived_sum(own, norm, (p1, p2, p3))
    search[...] = value
    put(message, value, squares(value))
    total[...] = wide(row)


def next_body(own, norm, p1, p2, p3, old, gamma, guess, search, message, step):
    value, row = arrived_sum(own, norm, (p1, p2, p3))
    alpha = gamma[0:1] / row
    ratio = per_frame(alpha / guess[0:1], VS)
    fresh = (1.0 - ratio) * old[...] + ratio * value
    search[...] = fresh
    put(message, fresh, squares(fresh))
    step[...] = wide(alpha)


def update_body(first, step, old, res, image, *refs):
    direction, volume, residual = refs[-3:]
    alpha = per_frame(step[0:1], VS)
    if first:
        along = old[...]
        volume[...] = alpha * along
    else:
        beta, way, vol = refs[:3]
        along = old[...] + per_frame(beta[0:1], VS) * way[...]
        volume[...] = vol[...] + alpha * along
    direction[...] = along
    residual[...] = res[...] - alpha[:, :RO] * image[...]


SIZE = 4 * RS


def part_of(j, message, turned, at):
    first = j % 2 * VS
    return jnp.dot(
        unstacked(message[:VROWS]),
        turned[first : first + VS, at : at + SIZE],
        preferred_element_type=F32,
    )


def product_body(j, message, turned, *refs):
    image = refs[-1]
    for at in range(0, NK * RAYS, SIZE):
        part = part_of(j, message, turned, at)
        if len(refs) > 1:
            part = part + refs[0][:, at : at + SIZE]
        image[:, at : at + SIZE] = part


def forward_body(j, message, turned, so_far, m1, m2, m3, out):
    row = jnp.zeros((1, LANES), F32)
    for m in (message, m1, m2, m3):
        row = row + row_of(m[VROWS:])
    rows = as_rows(row)
    for c in range(NC):
        out[c, NK * FH :] = rows
    for at in range(0, NK * RAYS, SIZE):
        part = (part_of(j, message, turned, at) + so_far[:, at : at + SIZE]).astype(BF)
        h, first = at // RAYS, at % RAYS // RS
        for c in range(SIZE // RS):
            out[first + c, h * FH : (h + 1) * FH] = part[:, c * RS : (c + 1) * RS]


def gathered(arrived):
    value = arrived[0].astype(F32)
    for c in range(1, NC):
        value = value + arrived[c].astype(F32)
    return unstacked(value[: NK * FH]), jnp.sum(value[NK * FH :], axis=0, keepdims=True)


def image_first_body(arrived, res, last, image, gamma, guess, message):
    value, row = gathered(arrived)
    image[...] = value
    gamma[...] = wide(row)
    about = last[0:1] / row
    about = jnp.where((about > 0.0) & (about < jnp.inf), about, 1.0)
    guess[...] = wide(about)
    put_all(message, res[...] - per_frame(about, RO) * value, squares(value))


def image_next_body(arrived, res, about, previous, last, image, gamma, beta, message):
    value, row = gathered(arrived)
    ratio = row / last[0:1]
    value = value + per_frame(ratio, RO) * previous[...]
    image[...] = value
    gamma[...] = wide(row)
    beta[...] = wide(ratio)
    put_all(message, res[...] - per_frame(about[0:1], RO) * value, squares(value))


def image_last_body(arrived, previous, last, image, gamma, beta, norm):
    value, row = gathered(arrived)
    ratio = row / last[0:1]
    value = value + per_frame(ratio, RO) * previous[...]
    image[...] = value
    gamma[...] = wide(row)
    beta[...] = wide(ratio)
    norm[...] = wide(squares(value))


def norm_body(mine, far, near, back, norms):
    total = mine[...] + far[...] + near[...] + back[...]
    for c in range(NC):
        norms[c] = total


def final_body(k, norms, gamma, search, beta, way, vol, res, image, mine, other, volume):
    total = norms[0, 0:1]
    for c in range(1, NC):
        total = total + norms[c, 0:1]
    alpha = per_frame(gamma[0:1] / total, VS)
    along = search[...] + per_frame(beta[0:1], VS) * way[...]
    volume[...] = vol[...] + alpha * along
    residual = res[...] - alpha[:, :RO] * image[...]
    mine[:, :VH] = volume[:, pl.ds(pl.multiple_of(k[0] * VH, VH), VH)]
    other[:, :VH] = volume[:, pl.ds(pl.multiple_of((1 - k[0]) * VH, VH), VH)]
    mine[:, VH:] = residual[:, :RS]
    other[:, VH:] = residual[:, RS:]


def finish_body(k, mine, other, volume, residual, turned):
    turned[pl.ds(pl.multiple_of(k[0] * FH, FH), FH)] = mine[...]
    turned[pl.ds(pl.multiple_of((1 - k[0]) * FH, FH), FH)] = other[...]
    whole = turned[...].T
    volume[...] = whole[:VH]
    residual[...] = whole[VH:]


def swapped(value, axis, by):
    return lax.ppermute(value, axis, [(i, i ^ by) for i in range(lax.axis_size(axis))])


def exchanged(parts, axis):
    return lax.all_to_all(parts, axis, split_axis=0, concat_axis=0, tiled=True)


LINE = (8, LANES)
COLUMN = (NC, NK * FH + PAD, RS)
SHARD = (VROWS + PAD, LANES)


def local(tiles, tile_row, tile_col, tile_count, sinogram):
    x = lax.axis_index("x").astype(jnp.int32).reshape(1)
    k = lax.axis_index("k").astype(jnp.int32).reshape(1)
    line = shape(LINE, F32)
    rays = shape((FH, RO), F32)
    voxels = shape((FH, VS), F32)
    column = shape(COLUMN, BF)
    shard = shape(SHARD, BF)

    table = jnp.concatenate(
        [tile_row[0], tile_col[0], jnp.broadcast_to(tile_count, tile_row.shape[1:])], axis=0
    )
    half = shape((FH, RS), F32)
    mine, other = kernel(
        turn_body, (half, half), (k, sinogram[0]), (pltpu.VMEM((FRAMES, RS), F32),)
    )
    table2 = swapped(table, "k", 1)
    other = swapped(other, "k", 1)
    stored, other, table2, x = lax.optimization_barrier((tiles[0, 0], other, table2, x))
    stored2 = swapped(stored, "k", 1)
    residual, message = kernel(start_body, (rays, column), (mine, other))
    arrived = exchanged(message, COL)
    dense = build(x, table, table2, stored, stored2, arrived)
    turned = (turned_half(0, dense), turned_half(1, dense))

    def backward_of(arrived):
        field, norm, p2 = kernel(
            gather_body, (shape((FH, NK * RAYS), BF), line, shard), (arrived, dense), limit=8
        )

        def piece(j, out):
            return kernel(functools.partial(piece_body, j), out, (field, norm, dense), limit=8)

        two = swapped(p2, "x", 2)
        p3 = piece(3, shard)
        three = swapped(p3, "x", 3)
        p1 = piece(1, shard)
        one = swapped(p1, "x", 1)
        return piece(0, voxels), norm, two, three, one

    def forward(message, update=None):
        return forward_of(message, update)

    def forward_of(message, update):
        two = swapped(message, "x", 2)
        three = swapped(message, "x", 3)
        one = swapped(message, "x", 1)
        whole = shape((FH, NK * RAYS), F32)

        def product(j, message, *so_far):
            return kernel(
                functools.partial(product_body, j),
                whole,
                (message, turned[j // 2], *so_far),
                limit=8,
            )

        image = product(0, message)
        updated = None
        if update is not None:
            updated = update()
        image = product(2, two, image)
        image = product(3, three, image)
        out = kernel(
            functools.partial(forward_body, 1),
            column,
            (one, turned[0], image, message, two, three),
            limit=8,
        )
        return exchanged(out, COL), updated

    search, shard_out, last = kernel(first_body, (voxels, shard, line), backward_of(arrived))
    image, gamma, guess, message = kernel(
        image_first_body, (rays, line, line, column), (forward(shard_out)[0], residual, last)
    )
    beta = direction = volume = None
    for step in range(1, ITERS):
        old = search
        search, shard_out, guess = kernel(
            next_body,
            (voxels, shard, line),
            (*backward_of(exchanged(message, COL)), old, gamma, guess),
        )
        state = (guess, old, residual, image)
        if step > 1:
            state += (beta, direction, volume)

        def update(state=state, first=step == 1):
            return kernel(functools.partial(update_body, first), (voxels, voxels, rays), state)

        arrived, (direction, volume, residual) = forward(shard_out, update)
        if step + 1 < ITERS:
            image, gamma, beta, message = kernel(
                image_next_body,
                (rays, line, line, column),
                (arrived, residual, guess, image, gamma),
            )
    image, gamma, beta, norm = kernel(
        image_last_body, (rays, line, line, line), (arrived, image, gamma)
    )
    others = tuple(swapped(norm, "x", j) for j in (2, 1, 3))
    norms = kernel(norm_body, shape((NC, *LINE), F32), (norm, *others))
    both = shape((FH, VH + RS), F32)
    mine, other = kernel(
        final_body,
        (both, both),
        (k, exchanged(norms, COL), gamma, search, beta, direction, volume, residual, image),
        (pltpu.VMEM((FH, VS), F32),),
    )
    volume, residual = kernel(
        finish_body,
        (shape((VH, FRAMES), F32), shape((RS, FRAMES), F32)),
        (k, mine, swapped(other, "k", 1)),
        (pltpu.VMEM((FRAMES, VH + RS), F32),),
    )
    return volume[None], residual[None]


def solution(mesh):
    finer = Mesh(mesh.devices.reshape(4, 2, 4, 4), ("x", "k", "y", "z"))
    placed = (
        P(ROW, COL, None, None, None),
        P(ROW, COL, None),
        P(ROW, COL, None),
        P(ROW, COL),
        P(ROW, COL, None),
    )
    return jax.shard_map(
        local,
        mesh=finer,
        in_specs=placed,
        out_specs=(P(COL, ROW, None), P(ROW, COL, None)),
        check_vma=False,
    )
```

```python
import functools

import jax
import jax.numpy as jnp
from jax import lax
from jax.experimental import pallas as pl
from jax.experimental.pallas import tpu as pltpu
from jax.sharding import Mesh
from jax.sharding import PartitionSpec as P


ROW = ("x", "k")
COL = ("y", "z")
NX, NK, NC = 4, 2, 16
TILE = 128
RAYS = 2048
VOX = 2048
FRAMES = 128
ITERS = 4
FH = FRAMES // NK
RS = RAYS // NC
RO = NK * RS
VS = VOX // NX
VH = VS // NK
VROWS = VS // 128 * FH
PAD = 8
LANES = 128
BF = jnp.bfloat16
F32 = jnp.float32


def vmem():
    return pl.BlockSpec(memory_space=pltpu.VMEM)


def smem():
    return pl.BlockSpec(memory_space=pltpu.SMEM)


def hbm():
    return pl.BlockSpec(memory_space=pltpu.HBM)


def shape(dims, dtype):
    return jax.ShapeDtypeStruct(dims, dtype)


def kernel(body, outs, ins, scratch=(), limit=4):
    return pl.pallas_call(
        body,
        out_shape=outs,
        in_specs=[smem() if a.dtype == jnp.int32 else vmem() for a in ins],
        out_specs=jax.tree.map(lambda _: vmem(), outs),
        scratch_shapes=list(scratch),
        compiler_params=pltpu.CompilerParams(vmem_limit_bytes=limit << 20),
    )(*ins)


def squares(values):
    total = values[:, :LANES] * values[:, :LANES]
    for i in range(LANES, values.shape[1], LANES):
        total += values[:, i : i + LANES] * values[:, i : i + LANES]
    square = jnp.concatenate([total, jnp.zeros((LANES - FH, LANES), F32)], axis=0)
    return jnp.sum(square.T, axis=0, keepdims=True)


def per_frame(row, width):
    column = jnp.broadcast_to(row, (LANES, LANES)).T[:FH]
    return jnp.concatenate([column] * (width // LANES), axis=1)


def as_rows(row):
    high = row.astype(BF).astype(F32)
    rest = row - high
    mid = rest.astype(BF).astype(F32)
    low = rest - mid
    i = lax.broadcasted_iota(jnp.int32, (PAD, LANES), 0)
    zero = jnp.zeros((PAD, LANES), F32)
    return jnp.where(i == 0, high, jnp.where(i == 1, mid, jnp.where(i == 2, low, zero))).astype(BF)


def row_of(rows):
    return jnp.sum(rows.astype(F32), axis=0, keepdims=True)


def wide(row):
    return jnp.broadcast_to(row, (8, LANES))


def stacked(values):
    return jnp.concatenate(
        [values[:, i : i + LANES] for i in range(0, values.shape[1], LANES)], axis=0
    )


def unstacked(rows):
    return jnp.concatenate([rows[i : i + FH] for i in range(0, rows.shape[0], FH)], axis=1)


def put(message, values, row):
    message[: message.shape[0] - PAD] = stacked(values.astype(BF))
    message[message.shape[0] - PAD :] = as_rows(row)


def put_all(message, values, row):
    part = stacked(values.astype(BF))
    rows = as_rows(row)
    for c in range(NC):
        message[c, : RO // LANES * FH] = part
        message[c, RO // LANES * FH :] = rows


def turn_body(k, sino, mine, other, turned):
    turned[...] = sino[...].T
    mine[...] = turned[pl.ds(pl.multiple_of(k[0] * FH, FH), FH)]
    other[...] = turned[pl.ds(pl.multiple_of((1 - k[0]) * FH, FH), FH)]


def start_body(mine, other, residual, message):
    values = jnp.concatenate([mine[...], other[...]], axis=1)
    residual[...] = values
    put_all(message, values, squares(values))


def build_body(x, table, table2, tiles, tiles2, after, dense, sem, sem2):
    halves = ((table, tiles, sem), (table2, tiles2, sem2))

    def copy(half, t):
        index, stored, done = halves[half]
        r = pl.multiple_of(index[0, t] * TILE + half * RAYS, TILE)
        piece = index[1, t] // (VS // TILE) ^ x[0]
        c = pl.multiple_of(piece * VS + index[1, t] % (VS // TILE) * TILE, TILE)
        return pltpu.make_async_copy(stored.at[t], dense.at[pl.ds(r, TILE), pl.ds(c, TILE)], done)

    for half in range(NK):

        def start(t, carry, half=half):
            copy(half, t).start()
            return carry

        dense[half * RAYS : (half + 1) * RAYS] = jnp.zeros((RAYS, VOX), BF)
        lax.fori_loop(0, halves[half][0][2, 0], start, 0)
    for half in range(NK):

        def wait(t, carry, half=half):
            copy(half, t).wait()
            return carry

        lax.fori_loop(0, halves[half][0][2, 0], wait, 0)


def build(x, table, table2, tiles, tiles2, after):
    return pl.pallas_call(
        build_body,
        name="build",
        out_shape=pltpu.VMEM((NK * RAYS, VOX), BF),
        in_specs=[smem(), smem(), smem(), hbm(), hbm(), vmem()],
        out_specs=vmem(),
        scratch_shapes=[pltpu.SemaphoreType.DMA(()), pltpu.SemaphoreType.DMA(())],
        compiler_params=pltpu.CompilerParams(vmem_limit_bytes=44 << 20),
    )(x, table, table2, tiles, tiles2, after)


def turned_body(half, dense, turned):
    def turn(j, carry):
        voxels = pl.ds(pl.multiple_of(j * TILE, TILE), TILE)
        here = pl.ds(pl.multiple_of(j * TILE + half * VOX // 2, TILE), TILE)
        for i in range(0, NK * RAYS, TILE):
            turned[voxels, i : i + TILE] = dense[i : i + TILE, here].T
        return carry

    lax.fori_loop(0, VOX // 2 // TILE, turn, 0)


def turned_half(half, dense):
    return pl.pallas_call(
        functools.partial(turned_body, half),
        out_shape=pltpu.VMEM((VOX // 2, NK * RAYS), BF),
        in_specs=[vmem()],
        out_specs=vmem(),
        compiler_params=pltpu.CompilerParams(vmem_limit_bytes=4 << 20),
    )(dense)


def gather_body(arrived, dense, field, norm, far):
    seen = arrived[0, NK * FH :].astype(F32)
    for c in range(NC):
        for h in range(NK):
            field[:, h * RAYS + c * RS : h * RAYS + (c + 1) * RS] = arrived[c, h * FH : (h + 1) * FH]
        if c:
            seen += arrived[c, NK * FH :].astype(F32)
    row = row_of(seen)
    norm[...] = wide(row)
    part = jnp.dot(field[...], dense[:, 2 * VS : 3 * VS], preferred_element_type=F32)
    put(far, part, row)


def piece_body(j, field, norm, dense, out):
    part = jnp.dot(field[...], dense[:, j * VS : (j + 1) * VS], preferred_element_type=F32)
    if j:
        put(out, part, norm[0:1])
    else:
        out[...] = part


def arrived_sum(own, norm, pieces):
    value = own[...]
    row = norm[0:1]
    for p in pieces:
        value = value + unstacked(p[:VROWS].astype(F32))
        row = row + row_of(p[VROWS:])
    return value, row


def first_body(own, norm, p1, p2, p3, search, message, total):
    value, row = arrived_sum(own, norm, (p1, p2, p3))
    search[...] = value
    put(message, value, squares(value))
    total[...] = wide(row)


def next_body(own, norm, p1, p2, p3, old, gamma, guess, search, message, step):
    value, row = arrived_sum(own, norm, (p1, p2, p3))
    alpha = gamma[0:1] / row
    ratio = per_frame(alpha / guess[0:1], VS)
    fresh = (1.0 - ratio) * old[...] + ratio * value
    search[...] = fresh
    put(message, fresh, squares(fresh))
    step[...] = wide(alpha)


def update_body(first, step, old, res, image, *refs):
    direction, volume, residual = refs[-3:]
    alpha = per_frame(step[0:1], VS)
    if first:
        along = old[...]
        volume[...] = alpha * along
    else:
        beta, way, vol = refs[:3]
        along = old[...] + per_frame(beta[0:1], VS) * way[...]
        volume[...] = vol[...] + alpha * along
    direction[...] = along
    residual[...] = res[...] - alpha[:, :RO] * image[...]


SIZE = 4 * RS


def part_of(j, message, turned, at):
    first = j % 2 * VS
    return jnp.dot(
        unstacked(message[:VROWS]),
        turned[first : first + VS, at : at + SIZE],
        preferred_element_type=F32,
    )


def product_body(j, message, turned, *refs):
    image = refs[-1]
    for at in range(0, NK * RAYS, SIZE):
        part = part_of(j, message, turned, at)
        if len(refs) > 1:
            part = part + refs[0][:, at : at + SIZE]
        image[:, at : at + SIZE] = part


def forward_body(j, message, turned, so_far, m1, m2, m3, out):
    row = jnp.zeros((1, LANES), F32)
    for m in (message, m1, m2, m3):
        row = row + row_of(m[VROWS:])
    rows = as_rows(row)
    for c in range(NC):
        out[c, NK * FH :] = rows
    for at in range(0, NK * RAYS, SIZE):
        part = (part_of(j, message, turned, at) + so_far[:, at : at + SIZE]).astype(BF)
        h, first = at // RAYS, at % RAYS // RS
        for c in range(SIZE // RS):
            out[first + c, h * FH : (h + 1) * FH] = part[:, c * RS : (c + 1) * RS]


def gathered(arrived):
    value = arrived[0].astype(F32)
    for c in range(1, NC):
        value = value + arrived[c].astype(F32)
    return unstacked(value[: NK * FH]), jnp.sum(value[NK * FH :], axis=0, keepdims=True)


def image_first_body(arrived, res, last, image, gamma, guess, message):
    value, row = gathered(arrived)
    image[...] = value
    gamma[...] = wide(row)
    about = last[0:1] / row
    about = jnp.where((about > 0.0) & (about < jnp.inf), about, 1.0)
    guess[...] = wide(about)
    put_all(message, res[...] - per_frame(about, RO) * value, squares(value))


def image_next_body(arrived, res, about, previous, last, image, gamma, beta, message):
    value, row = gathered(arrived)
    ratio = row / last[0:1]
    value = value + per_frame(ratio, RO) * previous[...]
    image[...] = value
    gamma[...] = wide(row)
    beta[...] = wide(ratio)
    put_all(message, res[...] - per_frame(about[0:1], RO) * value, squares(value))


def image_last_body(arrived, previous, last, image, gamma, beta, norms):
    value, row = gathered(arrived)
    ratio = row / last[0:1]
    value = value + per_frame(ratio, RO) * previous[...]
    image[...] = value
    gamma[...] = wide(row)
    beta[...] = wide(ratio)
    rows = as_rows(squares(value))
    for i in range(NX * NC):
        norms[i] = rows


def final_body(k, norms, gamma, search, beta, way, vol, res, image, mine, other, volume):
    total = norms[0].astype(F32)
    for i in range(1, NX * NC):
        total = total + norms[i].astype(F32)
    total = jnp.sum(total, axis=0, keepdims=True)
    alpha = per_frame(gamma[0:1] / total, VS)
    along = search[...] + per_frame(beta[0:1], VS) * way[...]
    volume[...] = vol[...] + alpha * along
    residual = res[...] - alpha[:, :RO] * image[...]
    mine[:, :VH] = volume[:, pl.ds(pl.multiple_of(k[0] * VH, VH), VH)]
    other[:, :VH] = volume[:, pl.ds(pl.multiple_of((1 - k[0]) * VH, VH), VH)]
    mine[:, VH:] = residual[:, :RS]
    other[:, VH:] = residual[:, RS:]


def finish_body(k, mine, other, volume, residual, turned):
    turned[pl.ds(pl.multiple_of(k[0] * FH, FH), FH)] = mine[...]
    turned[pl.ds(pl.multiple_of((1 - k[0]) * FH, FH), FH)] = other[...]
    whole = turned[...].T
    volume[...] = whole[:VH]
    residual[...] = whole[VH:]


def swapped(value, axis, by):
    return lax.ppermute(value, axis, [(i, i ^ by) for i in range(lax.axis_size(axis))])


def exchanged(parts, axis):
    return lax.all_to_all(parts, axis, split_axis=0, concat_axis=0, tiled=True)


LINE = (8, LANES)
COLUMN = (NC, NK * FH + PAD, RS)
SHARD = (VROWS + PAD, LANES)


def local(tiles, tile_row, tile_col, tile_count, sinogram):
    x = lax.axis_index("x").astype(jnp.int32).reshape(1)
    k = lax.axis_index("k").astype(jnp.int32).reshape(1)
    line = shape(LINE, F32)
    rays = shape((FH, RO), F32)
    voxels = shape((FH, VS), F32)
    column = shape(COLUMN, BF)
    shard = shape(SHARD, BF)

    table = jnp.concatenate(
        [tile_row[0], tile_col[0], jnp.broadcast_to(tile_count, tile_row.shape[1:])], axis=0
    )
    half = shape((FH, RS), F32)
    mine, other = kernel(
        turn_body, (half, half), (k, sinogram[0]), (pltpu.VMEM((FRAMES, RS), F32),)
    )
    table2 = swapped(table, "k", 1)
    other = swapped(other, "k", 1)
    stored, other, table2, x = lax.optimization_barrier((tiles[0, 0], other, table2, x))
    stored2 = swapped(stored, "k", 1)
    residual, message = kernel(start_body, (rays, column), (mine, other))
    arrived = exchanged(message, COL)
    dense = build(x, table, table2, stored, stored2, arrived)
    turned = (turned_half(0, dense), turned_half(1, dense))

    def backward_of(arrived):
        field, norm, p2 = kernel(
            gather_body, (shape((FH, NK * RAYS), BF), line, shard), (arrived, dense), limit=8
        )

        def piece(j, out):
            return kernel(functools.partial(piece_body, j), out, (field, norm, dense), limit=8)

        two = swapped(p2, "x", 2)
        p3 = piece(3, shard)
        three = swapped(p3, "x", 3)
        p1 = piece(1, shard)
        one = swapped(p1, "x", 1)
        return piece(0, voxels), norm, two, three, one

    def forward(message, update=None):
        return forward_of(message, update)

    def forward_of(message, update):
        two = swapped(message, "x", 2)
        three = swapped(message, "x", 3)
        one = swapped(message, "x", 1)
        whole = shape((FH, NK * RAYS), F32)

        def product(j, message, *so_far):
            return kernel(
                functools.partial(product_body, j),
                whole,
                (message, turned[j // 2], *so_far),
                limit=8,
            )

        image = product(0, message)
        updated = None
        if update is not None:
            updated = update()
        image = product(2, two, image)
        image = product(3, three, image)
        out = kernel(
            functools.partial(forward_body, 1),
            column,
            (one, turned[0], image, message, two, three),
            limit=8,
        )
        return exchanged(out, COL), updated

    search, shard_out, last = kernel(first_body, (voxels, shard, line), backward_of(arrived))
    image, gamma, guess, message = kernel(
        image_first_body, (rays, line, line, column), (forward(shard_out)[0], residual, last)
    )
    beta = direction = volume = None
    for step in range(1, ITERS):
        old = search
        search, shard_out, guess = kernel(
            next_body,
            (voxels, shard, line),
            (*backward_of(exchanged(message, COL)), old, gamma, guess),
        )
        state = (guess, old, residual, image)
        if step > 1:
            state += (beta, direction, volume)

        def update(state=state, first=step == 1):
            return kernel(functools.partial(update_body, first), (voxels, voxels, rays), state)

        arrived, (direction, volume, residual) = forward(shard_out, update)
        if step + 1 < ITERS:
            image, gamma, beta, message = kernel(
                image_next_body,
                (rays, line, line, column),
                (arrived, residual, guess, image, gamma),
            )
    image, gamma, beta, norms = kernel(
        image_last_body,
        (rays, line, line, shape((NX * NC, PAD, LANES), BF)),
        (arrived, image, gamma),
    )
    both = shape((FH, VH + RS), F32)
    mine, other = kernel(
        final_body,
        (both, both),
        (k, exchanged(norms, ("x", *COL)), gamma, search, beta, direction, volume, residual, image),
        (pltpu.VMEM((FH, VS), F32),),
    )
    volume, residual = kernel(
        finish_body,
        (shape((VH, FRAMES), F32), shape((RS, FRAMES), F32)),
        (k, mine, swapped(other, "k", 1)),
        (pltpu.VMEM((FRAMES, VH + RS), F32),),
    )
    return volume[None], residual[None]


def solution(mesh):
    finer = Mesh(mesh.devices.reshape(4, 2, 4, 4), ("x", "k", "y", "z"))
    placed = (
        P(ROW, COL, None, None, None),
        P(ROW, COL, None),
        P(ROW, COL, None),
        P(ROW, COL),
        P(ROW, COL, None),
    )
    return jax.shard_map(
        local,
        mesh=finer,
        in_specs=placed,
        out_specs=(P(COL, ROW, None), P(ROW, COL, None)),
        check_vma=False,
    )
```
